128 devices in a mesh: gx: 4 (over x_hi, core), gy: 4 (over y), gz: 8 (over z, x_lo).
Axes of the slice: x: 4 (x_hi: 2, x_lo: 2; x = x_hi * 2 + x_lo), y: 4, z: 4, core: 2. Of those that a mesh axis runs over, the one named last changes fastest.
Arguments:
- field: float32 [64, 1024, 1024], P('gx', 'gy', 'gz'), may hold values from -6 to 6
- source: float32 [64, 1024, 1024], P('gx', 'gy', 'gz'), may hold values from -6 to 6
Outputs:
- smoothed: float32 [64, 1024, 1024], P('gx', 'gy', 'gz')
The draws below stay inside these ranges and needn't reach their ends.
All inputs are finite; a program needn't handle non-finite values.
Results may differ from the reference program's by a relative error of at most 0.00002.
Values sent between devices are 32-bit elements; how exact they have to be, the bound alone decides.
A program may use at most 64 MiB of HBM per device.

```python
import jax
import jax.numpy as jnp

SWEEPS = 3
NX = 64
NY = 1024
NZ = 1024


def block_levels(key, shape, split, least, top_value):
    def one(position, parts):
        draws = jax.random.uniform(jax.random.fold_in(jax.random.fold_in(key, 6), position), (parts,), jnp.float32, least / len(split), top_value / len(split))
        return jnp.repeat(jnp.exp(draws), shape[position] // parts).reshape((-1,) + (1,) * (len(shape) - position - 1))

    loudness = one(*split[0])
    for cut in split[1:]:
        loudness = loudness * one(*cut)
    return loudness


def bell_draw(own_key, shape, spread, most, shards=(), held_as=jnp.bfloat16):
    entries = jax.random.normal(own_key, shape, jnp.float32) * spread
    if len(shards) > 0:
        entries = block_levels(own_key, shape, shards, -0.22, 0.18) * entries
    return jnp.clip(entries, min=-most, max=most).astype(held_as)


def setup_inputs(seed: int = 0) -> dict:
    key_of = jax.random.split(jax.random.key(seed), 3)
    field = bell_draw(key_of[0], (NX, NY, NZ), 1.0, 6.0, ((0, 4), (1, 4), (2, 8)), jnp.float32)
    source = bell_draw(key_of[1], (NX, NY, NZ), 1.0, 6.0, ((0, 4), (1, 4), (2, 8)), jnp.float32)
    return dict(field=field, source=source)


def relax(values, source, parity, colour):
    padded = jnp.pad(values, ((1, 1), (0, 0), (0, 0)))
    beside = padded[2:] + padded[:-2]
    beside = beside + jnp.roll(values, -1, 1) + jnp.roll(values, 1, 1)
    beside = beside + jnp.roll(values, -1, 2) + jnp.roll(values, 1, 2)
    return jnp.where(parity == colour, (source + beside) / 6.0, values)


def reference(field, source):
    nx, ny, nz = field.shape
    parity = (jnp.arange(nx, dtype=jnp.int32)[:, None, None] + jnp.arange(ny, dtype=jnp.int32)[None, :, None] + jnp.arange(nz, dtype=jnp.int32)[None, None, :]) % 2
    values = field
    for sweep in range(SWEEPS):
        values = relax(values, source, parity, 0)
        values = relax(values, source, parity, 1)
    return values
```

```python
import functools
import itertools

import jax
import jax.numpy as jnp
from jax import lax
from jax.experimental import pallas as pl
from jax.experimental.pallas import tpu as pltpu
from jax.sharding import PartitionSpec as P

MESH = pl.DeviceIdType.MESH
SWEEPS = 3
NQ, NY, NZ = 8, 256, 128
TILES = NY // 8
TOP = 16
ROWS = NY + 2 * TOP
SIXTH = 1.0 / 6.0

EDGES = [d for d in itertools.product((-1, 0, 1), repeat=3) if sum(map(abs, d)) == 2]
FACES = [(0, 0, 1), (0, 0, -1), (0, 1, 0), (0, -1, 0), (1, 0, 0), (-1, 0, 0)]
MESSAGES = [d for d in EDGES if d[0] == 0] + [d for d in EDGES if d[0]] + FACES
Z_FACES = [(0, 0, 1), (0, 0, -1)]


def when(cond, f):
    if cond is None:
        f()
    else:
        pl.when(cond)(f)


def kernel(
    field, source, out,
    fld, src, blk, red, sred, sblk, ql, qr, qs, sql, sqr, sqs, rql, rqr,
    load_sem, store_sem, send_sem, recv_sem, ssend_sem, srecv_sem,
):
    gx, gy, gz = (lax.axis_index(a) for a in ("gx", "gy", "gz"))
    nx, ny, nz = (lax.axis_size(a) for a in ("gx", "gy", "gz"))
    low_wall, high_wall = gx == 0, gx == nx - 1

    def device(d):
        return {
            "gx": gx + d[0],
            "gy": lax.rem(gy + d[1] + ny, ny),
            "gz": lax.rem(gz + d[2] + nz, nz),
        }

    def exists(d):
        if d[0] > 0:
            return gx < nx - 1
        if d[0] < 0:
            return gx > 0
        return None

    def opposite(d):
        return tuple(-v for v in d)

    own = pl.ds(TOP, NY)

    def refs(r, d):
        dx, dy, dz = d
        if dz == 0:
            sp, dp = ((8, 0) if dx > 0 else (1, 9)) if dx else (pl.ds(1, NQ), pl.ds(1, NQ))
            sr, dr = ((TOP + NY - 8, TOP - 8) if dy > 0 else (TOP, TOP + NY)) if dy else (TOP, TOP)
            n = 8 if dy else NY
            return blk.at[r, sp, pl.ds(sr, n)], blk.at[r, dp, pl.ds(dr, n)]
        col, dst = (0, ql) if dz > 0 else (2, qr)
        if dx:
            return qs.at[r, col], dst.at[r, 0 if dx > 0 else 3, pl.ds(8, 16)]
        if dy:
            sr, dr = (8, 0) if dy > 0 else (0, 24)
            return qs.at[r, col, pl.ds(sr, 8)], dst.at[r, 1, pl.ds(dr, 8)]
        return qs.at[r, pl.ds(col, 2)], dst.at[r, pl.ds(1, 2), pl.ds(8, 16)]

    def message(r, m):
        d = MESSAGES[m]
        s, t = refs(r, d)
        return pltpu.make_async_remote_copy(
            src_ref=s, dst_ref=t, send_sem=send_sem.at[m], recv_sem=recv_sem.at[r, m],
            device_id=device(d), device_id_type=MESH,
        )

    def smessage(m):
        d = FACES[m]
        dx, dy, dz = d
        if dz:
            s, t = (sqs.at[0], sql) if dz > 0 else (sqs.at[1], sqr)
        else:
            sp, dp = ((8, 0) if dx > 0 else (1, 9)) if dx else (pl.ds(1, NQ), pl.ds(1, NQ))
            sr, dr = ((TOP + NY - 8, TOP - 8) if dy > 0 else (TOP, TOP + NY)) if dy else (TOP, TOP)
            n = 8 if dy else NY
            s, t = sred.at[sp, pl.ds(sr, n)], sred.at[dp, pl.ds(dr, n)]
        return pltpu.make_async_remote_copy(
            src_ref=s, dst_ref=t, send_sem=ssend_sem.at[m], recv_sem=srecv_sem.at[m],
            device_id=device(d), device_id_type=MESH,
        )

    def each(make, dirs, what, select=None):
        for m, d in enumerate(dirs):
            if select is not None and d not in select:
                continue
            if what == "start":
                when(exists(d), lambda m=m: make(m).start())
            elif what == "sent":
                when(exists(d), lambda m=m: make(m).wait_send())
            else:
                when(exists(opposite(d)), lambda m=m: make(m).wait_recv())

    barrier = pltpu.get_barrier_semaphore()
    for d in MESSAGES:
        when(exists(d), lambda d=d: pl.semaphore_signal(barrier, inc=1, device_id=device(d), device_id_type=MESH))

    def load(array, buffer, half, n):
        planes = pl.ds(4 * n, 4)
        return pltpu.make_async_copy(array.at[planes], buffer.at[planes], load_sem.at[half, n])

    for n in range(4):
        load(field, fld, 0, n).start()
    for n in range(4):
        load(source, src, 1, n).start()

    lane = lax.broadcasted_iota(jnp.int32, (8, NZ), 1)
    sub = lax.broadcasted_iota(jnp.int32, (8, NZ), 0)
    odd = lax.rem(lane + sub, 2) == 1
    first, last = lane == 0, lane == NZ - 1

    def roll(x, shift):
        return pltpu.roll(x, shift, 1)

    def extract(value, place, accs, cols):
        hit = lane == place
        return [
            jnp.where(hit, roll(value, lax.rem(place - c + 2 * NZ, NZ)), acc)
            for c, acc in zip(cols, accs)
        ]

    zero = jnp.zeros((ROWS, NZ), jnp.float32)
    red[0] = zero
    red[9] = zero

    def wall(pair, plane):
        for r in range(SWEEPS):
            blk[r, pair] = zero
            ql[r, plane] = jnp.zeros((32, NZ), jnp.float32)
            qr[r, plane] = jnp.zeros((32, NZ), jnp.float32)

    pl.when(low_wall)(lambda: wall(0, 0))
    pl.when(high_wall)(lambda: wall(9, 3))

    COLS = (127, 126, 0, 1)

    def pack_field(q, accs):
        accs = [list(a) for a in accs]
        for t in range(TILES):
            rows = pl.ds(8 * t, 8)
            value = jnp.where(odd, fld[2 * q, rows], fld[2 * q + 1, rows])
            blk[0, q + 1, pl.ds(TOP + 8 * t, 8)] = value
            v, a = divmod(t, 16)
            accs[v] = extract(value, 8 * a + q, accs[v], COLS)
        return tuple(tuple(a) for a in accs)

    blank = jnp.zeros((8, NZ), jnp.float32)
    accs = tuple((blank,) * 4 for _ in range(2))
    for n in range(4):
        load(field, fld, 0, n).wait()
        accs = lax.fori_loop(2 * n, 2 * n + 2, pack_field, accs)
    for v in range(2):
        for c in range(4):
            qs[0, c, pl.ds(8 * v, 8)] = accs[v][c]

    walls = jnp.where(jnp.logical_or(low_wall, high_wall), 1, 0)
    pl.semaphore_wait(barrier, len(MESSAGES) - 5 * walls)
    each(functools.partial(message, 0), MESSAGES, "start")

    def pack_source(q, accs):
        accs = [list(a) for a in accs]
        for t in range(TILES):
            rows = pl.ds(8 * t, 8)
            even_plane, odd_plane = src[2 * q, rows], src[2 * q + 1, rows]
            value = jnp.where(odd, odd_plane, even_plane)
            sred[q + 1, pl.ds(TOP + 8 * t, 8)] = value
            sblk[q, rows] = jnp.where(odd, even_plane, odd_plane)
            v, a = divmod(t, 16)
            accs[v] = extract(value, 8 * a + q, accs[v], (127, 0))
        return tuple(tuple(a) for a in accs)

    accs = tuple((blank,) * 2 for _ in range(2))
    for n in range(4):
        load(source, src, 1, n).wait()
        accs = lax.fori_loop(2 * n, 2 * n + 2, pack_source, accs)
    for v in range(2):
        for c in range(2):
            sqs[c, pl.ds(8 * v, 8)] = accs[v][c]
    each(smessage, FACES, "start")

    def column(r, side, edges):
        q, s, o, near = (ql, sql, rql, 2) if side == 0 else (qr, sqr, rqr, 0)
        turned = lax.rem(sub + (1 - side), 2) == 1
        for v in range(2):
            here = pl.ds(8 * v + 8, 8)
            c = q[r, 1, here]
            before = q[r, 1, pl.ds(8 * v, 8)] if edges or v == 1 else c
            after = q[r, 1, pl.ds(8 * v + 16, 8)] if edges or v == 0 else c
            wrap = jnp.where(lane < 8, roll(before, 8), roll(c, 8))
            total = c + jnp.where(sub == 0, pltpu.roll(wrap, 1, 0), pltpu.roll(c, 1, 0))
            wrap = jnp.where(lane >= 120, roll(after, 120), roll(c, 120))
            total = total + jnp.where(sub == 7, pltpu.roll(wrap, 7, 0), pltpu.roll(c, 7, 0))
            up, down = roll(c, 127), roll(c, 1)
            if edges:
                up = jnp.where(lax.rem(lane, 8) == 7, roll(q[r, 3, here], 7), up)
                down = jnp.where(lax.rem(lane, 8) == 0, roll(q[r, 0, here], 121), down)
            total = total + jnp.where(turned, up, down)
            rows = pl.ds(8 * v, 8)
            total = total + q[r, 2, here] + qs[r, near, rows] + s[rows]
            o[rows] = total * SIXTH

    def around(ref, lead, row, left, right, place):
        c = ref[(*lead, pl.ds(row, 8))]
        total = c + ref[(*lead, pl.ds(row - 1, 8))] + ref[(*lead, pl.ds(row + 1, 8))]
        ins_left = roll(left, lax.rem(NZ - place, NZ))
        ins_right = roll(right, NZ - 1 - place)
        total = total + jnp.where(first, ins_left, roll(c, 1))
        return total + jnp.where(last, ins_right, roll(c, NZ - 1))

    def red_pair(r, q, tiles):
        plane = jnp.where(q < 0, 0, jnp.where(q > 7, 3, 1))
        slot = jnp.bitwise_and(q, 7)
        above, below = jnp.minimum(q + 2, 9), jnp.maximum(q, 0)
        for t in tiles:
            row = TOP + 8 * t
            v, a = divmod(t, 16)
            here = pl.ds(8 * v + 8, 8)
            total = around(blk, (r, q + 1), row, ql[r, plane, here], qr[r, plane, here], 8 * a + slot)
            rows = pl.ds(row, 8)
            total = total + jnp.where(odd, blk[r, above, rows], blk[r, below, rows])
            red[q + 1, rows] = (total + sred[q + 1, rows]) * SIXTH

    def black_pair(r, q, tiles, accs):
        accs = [list(a) for a in accs]
        for t in tiles:
            row = TOP + 8 * t
            v, a = divmod(t, 16)
            here = pl.ds(8 * v, 8)
            total = around(red, (q + 1,), row, rql[here], rqr[here], 8 * a + q)
            rows = pl.ds(row, 8)
            total = total + jnp.where(odd, red[q, rows], red[q + 2, rows])
            value = (total + sblk[q, pl.ds(8 * t, 8)]) * SIXTH
            blk[r + 1, q + 1, rows] = value
            accs[v] = extract(value, 8 * a + q, accs[v], COLS)
        return tuple(tuple(a) for a in accs)

    def sweep(r, carry):
        here = functools.partial(message, r)
        each(here, MESSAGES, "arrived", Z_FACES)

        @pl.when(r == 0)
        def _():
            each(smessage, FACES, "arrived", Z_FACES)

        column(r, 0, False)
        column(r, 1, False)

        def red_inner(q, c):
            red_pair(r, q, range(1, TILES - 1))
            return c

        lax.fori_loop(1, 7, red_inner, 0)
        accs = tuple((blank,) * 4 for _ in range(2))
        accs = lax.fori_loop(
            2, 6, lambda q, accs: black_pair(r, q, range(2, TILES - 2), accs), accs
        )

        rest = [d for d in MESSAGES if d not in Z_FACES]
        each(here, MESSAGES, "arrived", rest)

        @pl.when(r == 0)
        def _():
            each(smessage, FACES, "arrived", [d for d in FACES if d not in Z_FACES])

        each(here, MESSAGES, "sent")
        column(r, 0, True)
        column(r, 1, True)

        def red_outer(n, c):
            red_pair(r, n - 1 + jnp.where(n >= 2, 6, 0), range(TILES))
            return c

        lax.fori_loop(jnp.where(low_wall, 1, 0), jnp.where(high_wall, 3, 4), red_outer, 0)

        def red_ends(q, c):
            red_pair(r, q, (-1, 0, TILES - 1, TILES))
            return c

        lax.fori_loop(0, NQ, red_ends, 0)
        accs = lax.fori_loop(
            2, 6, lambda q, accs: black_pair(r, q, (0, 1, TILES - 2, TILES - 1), accs), accs
        )
        accs = lax.fori_loop(
            0, 4,
            lambda n, accs: black_pair(r, n + jnp.where(n >= 2, 4, 0), range(TILES), accs),
            accs,
        )
        for v in range(2):
            for c in range(4):
                qs[r + 1, c, pl.ds(8 * v, 8)] = accs[v][c]

        @pl.when(r < SWEEPS - 1)
        def _():
            each(functools.partial(message, r + 1), MESSAGES, "start")

        return carry

    lax.fori_loop(0, SWEEPS, sweep, 0)
    each(smessage, FACES, "sent")

    def store(q):
        planes = pl.ds(2 * q, 2)
        return pltpu.make_async_copy(fld.at[planes], out.at[planes], store_sem.at[q])

    def unpack(q, c):
        for t in range(TILES):
            rows, mine = pl.ds(TOP + 8 * t, 8), pl.ds(8 * t, 8)
            x, y = red[q + 1, rows], blk[SWEEPS, q + 1, rows]
            fld[2 * q, mine] = jnp.where(odd, y, x)
            fld[2 * q + 1, mine] = jnp.where(odd, x, y)
        store(q).start()
        return c

    lax.fori_loop(0, NQ, unpack, 0)

    def stored(q, c):
        store(q).wait()
        return c

    lax.fori_loop(0, NQ, stored, 0)


def on_device(field, source):
    f32 = jnp.float32
    dma = pltpu.SemaphoreType.DMA
    return pl.pallas_call(
        kernel,
        name="smooth",
        out_shape=jax.ShapeDtypeStruct(field.shape, f32),
        in_specs=[pl.BlockSpec(memory_space=pl.ANY)] * 2,
        out_specs=pl.BlockSpec(memory_space=pl.ANY),
        scratch_shapes=[
            pltpu.VMEM((2 * NQ, NY, NZ), f32),
            pltpu.VMEM((2 * NQ, NY, NZ), f32),
            pltpu.VMEM((SWEEPS + 1, NQ + 2, ROWS, NZ), f32),
            pltpu.VMEM((NQ + 2, ROWS, NZ), f32),
            pltpu.VMEM((NQ + 2, ROWS, NZ), f32),
            pltpu.VMEM((NQ, NY, NZ), f32),
            pltpu.VMEM((SWEEPS, 4, 32, NZ), f32),
            pltpu.VMEM((SWEEPS, 4, 32, NZ), f32),
            pltpu.VMEM((SWEEPS + 1, 4, 16, NZ), f32),
            pltpu.VMEM((16, NZ), f32),
            pltpu.VMEM((16, NZ), f32),
            pltpu.VMEM((2, 16, NZ), f32),
            pltpu.VMEM((16, NZ), f32),
            pltpu.VMEM((16, NZ), f32),
            dma((2, 4)),
            dma((NQ,)),
            dma((len(MESSAGES),)),
            dma((SWEEPS, len(MESSAGES))),
            dma((len(FACES),)),
            dma((len(FACES),)),
        ],
        compiler_params=pltpu.CompilerParams(collective_id=0, has_side_effects=True),
    )(field, source)


def solution(mesh):
    spec = P("gx", "gy", "gz")
    return jax.shard_map(
        on_device, mesh=mesh, in_specs=(spec, spec), out_specs=spec, check_vma=False
    )
```

```python
import functools
import itertools

import jax
import jax.numpy as jnp
from jax import lax
from jax.experimental import pallas as pl
from jax.experimental.pallas import tpu as pltpu
from jax.sharding import PartitionSpec as P

MESH = pl.DeviceIdType.MESH
SWEEPS = 3
NQ, NY, NZ = 8, 256, 128
TILES = NY // 8
TOP = 16
ROWS = NY + 2 * TOP
VECS = TILES // 8
COLS = 8 * VECS
SIXTH = 1.0 / 6.0

EDGES = [d for d in itertools.product((-1, 0, 1), repeat=3) if sum(map(abs, d)) == 2]
FACES = [(0, 0, 1), (0, 0, -1), (0, 1, 0), (0, -1, 0), (1, 0, 0), (-1, 0, 0)]
MESSAGES = [d for d in EDGES if d[0] == 0] + [d for d in EDGES if d[0]] + FACES
Z_FACES = [(0, 0, 1), (0, 0, -1)]


def when(cond, f):
    if cond is None:
        f()
    else:
        pl.when(cond)(f)


def kernel(
    field, source, out,
    fld, src, blk, red, sred, sblk, ql, qr, qlo, qhi, sql, sqr, sqlo, sqhi, ins, xins, rins,
    load_sem, store_sem, send_sem, recv_sem, ssend_sem, srecv_sem,
):
    gx, gy, gz = (lax.axis_index(a) for a in ("gx", "gy", "gz"))
    nx, ny, nz = (lax.axis_size(a) for a in ("gx", "gy", "gz"))
    low_wall, high_wall = gx == 0, gx == nx - 1

    def device(d):
        return {
            "gx": gx + d[0],
            "gy": lax.rem(gy + d[1] + ny, ny),
            "gz": lax.rem(gz + d[2] + nz, nz),
        }

    def exists(d):
        if d[0] > 0:
            return gx < nx - 1
        if d[0] < 0:
            return gx > 0
        return None

    def opposite(d):
        return tuple(-v for v in d)

    def block_slices(d):
        dx, dy, _ = d
        sp, dp = ((8, 0) if dx > 0 else (1, 9)) if dx else (pl.ds(1, NQ), pl.ds(1, NQ))
        sr, dr = ((TOP + NY - 8, TOP - 8) if dy > 0 else (TOP, TOP + NY)) if dy else (TOP, TOP)
        n = 8 if dy else NY
        return (sp, pl.ds(sr, n)), (dp, pl.ds(dr, n))

    def refs(r, d):
        dx, dy, dz = d
        if dz == 0:
            s, t = block_slices(d)
            return blk.at[(r, *s)], blk.at[(r, *t)]
        col, dst = (qhi, ql) if dz > 0 else (qlo, qr)
        own = pl.ds(8, COLS)
        if dx:
            return col.at[r], dst.at[r, 0 if dx > 0 else 2, own]
        if dy:
            sr, dr = (COLS - 8, 0) if dy > 0 else (0, COLS + 8)
            return col.at[r, pl.ds(sr, 8)], dst.at[r, 1, pl.ds(dr, 8)]
        return col.at[r], dst.at[r, 1, own]

    def message(r, m):
        d = MESSAGES[m]
        s, t = refs(r, d)
        return pltpu.make_async_remote_copy(
            src_ref=s, dst_ref=t, send_sem=send_sem.at[m], recv_sem=recv_sem.at[r, m],
            device_id=device(d), device_id_type=MESH,
        )

    def smessage(m):
        d = FACES[m]
        if d[2]:
            s, t = (sqhi, sql) if d[2] > 0 else (sqlo, sqr)
        else:
            s, t = block_slices(d)
            s, t = sred.at[s], sred.at[t]
        return pltpu.make_async_remote_copy(
            src_ref=s, dst_ref=t, send_sem=ssend_sem.at[m], recv_sem=srecv_sem.at[m],
            device_id=device(d), device_id_type=MESH,
        )

    def each(make, dirs, what, select=None):
        for m, d in enumerate(dirs):
            if select is not None and d not in select:
                continue
            if what == "start":
                when(exists(d), lambda m=m: make(m).start())
            elif what == "sent":
                when(exists(d), lambda m=m: make(m).wait_send())
            else:
                when(exists(opposite(d)), lambda m=m: make(m).wait_recv())

    barrier = pltpu.get_barrier_semaphore()
    for d in MESSAGES:
        when(exists(d), lambda d=d: pl.semaphore_signal(barrier, inc=1, device_id=device(d), device_id_type=MESH))

    def load(array, buffer, half, n):
        planes = pl.ds(4 * n, 4)
        return pltpu.make_async_copy(array.at[planes], buffer.at[planes], load_sem.at[half, n])

    for n in range(4):
        load(field, fld, 0, n).start()
    for n in range(4):
        load(source, src, 1, n).start()

    lane = lax.broadcasted_iota(jnp.int32, (8, NZ), 1)
    sub = lax.broadcasted_iota(jnp.int32, (8, NZ), 0)
    odd = jnp.bitwise_and(lane + sub, 1) == 1
    even_lane = jnp.bitwise_and(lane, 1) == 0
    first, last = lane == 0, lane == NZ - 1
    group = jnp.bitwise_and(lane, 15)
    half = jnp.right_shift(lane, 1)
    half_after = jnp.bitwise_and(half - 1, NZ // 2 - 1)

    def roll(x, shift):
        return pltpu.roll(x, shift, 1)

    def slot(t, q):
        return 8 * (t % 8) + q

    def collect(lo, hi, lead, t, q, value):
        m = slot(t, q)
        turned = roll(value, jnp.bitwise_and(2 * m + 2, NZ - 1))
        rows = pl.ds(8 * (t // 8), 8)
        hi[(*lead, rows)] = jnp.where(half == m, turned, hi[(*lead, rows)])
        lo[(*lead, rows)] = jnp.where(half_after == m, turned, lo[(*lead, rows)])

    def settle(lo, lead):
        for v in range(VECS):
            rows = pl.ds(8 * v, 8)
            lo[(*lead, rows)] = roll(lo[(*lead, rows)], NZ - 2)

    zero = jnp.zeros((ROWS, NZ), jnp.float32)

    def wall(pair, plane):
        for r in range(SWEEPS):
            blk[r, pair] = zero
            ql[r, plane] = jnp.zeros((COLS + 16, NZ), jnp.float32)
            qr[r, plane] = jnp.zeros((COLS + 16, NZ), jnp.float32)
        sred[pair] = zero

    pl.when(low_wall)(lambda: wall(0, 0))
    pl.when(high_wall)(lambda: wall(9, 2))
    inside = jnp.where(odd, jnp.where(low_wall, 0.0, SIXTH), jnp.where(high_wall, 0.0, SIXTH))

    def pack_field(q, c):
        for t in range(TILES):
            rows = pl.ds(8 * t, 8)
            value = jnp.where(odd, fld[2 * q, rows], fld[2 * q + 1, rows])
            blk[0, q + 1, pl.ds(TOP + 8 * t, 8)] = value
            collect(qlo, qhi, (0,), t, q, value)
        return c

    for n in range(4):
        load(field, fld, 0, n).wait()
        lax.fori_loop(2 * n, 2 * n + 2, pack_field, 0)
    settle(qlo, (0,))

    walls = jnp.where(jnp.logical_or(low_wall, high_wall), 1, 0)
    pl.semaphore_wait(barrier, len(MESSAGES) - 5 * walls)
    each(functools.partial(message, 0), MESSAGES, "start")

    def pack_source(q, c):
        for t in range(TILES):
            rows = pl.ds(8 * t, 8)
            even_plane, odd_plane = src[2 * q, rows], src[2 * q + 1, rows]
            value = jnp.where(odd, odd_plane, even_plane)
            sred[q + 1, pl.ds(TOP + 8 * t, 8)] = value
            sblk[q, rows] = jnp.where(odd, even_plane, odd_plane)
            collect(sqlo, sqhi, (), t, q, value)
        return c

    for n in range(4):
        load(source, src, 1, n).wait()
        lax.fori_loop(2 * n, 2 * n + 2, pack_source, 0)
    settle(sqlo, ())
    each(smessage, FACES, "start")

    def columns(r, edges):
        for v in range(-1, VECS + 1) if edges else range(VECS):
            rows = pl.ds(8 * v + 8, 8)
            ins[rows] = jnp.where(even_lane, qr[r, 1, rows], ql[r, 1, rows])
        for v in range(VECS):
            here, rows = pl.ds(8 * v + 8, 8), pl.ds(8 * v, 8)
            c = ins[here]
            before = ins[rows] if edges or v > 0 else c
            after = ins[pl.ds(8 * v + 16, 8)] if edges or v < VECS - 1 else c
            back = roll(jnp.where(lane >= NZ - 16, before, c), 16)
            ahead = roll(jnp.where(lane < 16, after, c), NZ - 16)
            total = c + jnp.where(sub == 0, pltpu.roll(back, 1, 0), pltpu.roll(c, 1, 0))
            total = total + jnp.where(sub == 7, pltpu.roll(ahead, 7, 0), pltpu.roll(c, 7, 0))
            up, down = roll(c, NZ - 2), roll(c, 2)
            if edges:
                above = jnp.where(even_lane, qr[r, 2, here], ql[r, 2, here])
                below = jnp.where(even_lane, qr[r, 0, here], ql[r, 0, here])
                up = jnp.where(group >= 14, roll(above, 14), up)
                down = jnp.where(group < 2, roll(below, NZ - 14), down)
                xins[rows] = jnp.where(odd, above, roll(below, NZ - 14))
            total = total + jnp.where(odd, up, down)
            left, right = ql[r, 1, here] + qlo[r, rows], qr[r, 1, here] + qhi[r, rows]
            total = total + jnp.where(even_lane, roll(right, NZ - 1), roll(left, 1))
            total = total + jnp.where(even_lane, sqr[rows], sql[rows])
            rins[rows] = total * SIXTH

    def beside(c, edge, m):
        edge = roll(edge, NZ - 1 - 2 * m)
        return jnp.where(first, edge, roll(c, 1)) + jnp.where(last, edge, roll(c, NZ - 1))

    def around(ref, lead, row, edge, m):
        c = ref[(*lead, pl.ds(row, 8))]
        total = c + ref[(*lead, pl.ds(row - 1, 8))] + ref[(*lead, pl.ds(row + 1, 8))]
        return total + beside(c, edge, m)

    def red_tile(r, q, t):
        rows = pl.ds(TOP + 8 * t, 8)
        total = around(blk, (r, q + 1), TOP + 8 * t, ins[pl.ds(8 * (t // 8) + 8, 8)], slot(t, q))
        total = total + jnp.where(odd, blk[r, q + 2, rows], blk[r, q, rows])
        red[q + 1, rows] = (total + sred[q + 1, rows]) * SIXTH

    def halo_tiles(r):
        for t in range(TILES):
            row = TOP + 8 * t
            rows = pl.ds(row, 8)
            low, high = blk[r, 0, rows], blk[r, 9, rows]
            c, far = jnp.where(odd, high, low), jnp.where(odd, low, high)
            total = jnp.where(odd, blk[r, 0, pl.ds(row - 1, 8)], blk[r, 9, pl.ds(row - 1, 8)])
            total = total + jnp.where(odd, blk[r, 0, pl.ds(row + 1, 8)], blk[r, 9, pl.ds(row + 1, 8)])
            total = total + beside(c, xins[pl.ds(8 * (t // 8), 8)], slot(t, 0))
            total = total + far + jnp.where(odd, blk[r, 1, rows], blk[r, 8, rows])
            total = total + jnp.where(odd, sred[0, rows], sred[9, rows])
            red[0, rows] = total * inside

    def black_tile(r, q, t, final):
        rows = pl.ds(TOP + 8 * t, 8)
        total = around(red, (q + 1,), TOP + 8 * t, rins[pl.ds(8 * (t // 8), 8)], slot(t, q))
        above = (0 if q == NQ - 1 else q + 2) if isinstance(q, int) else q + 2
        total = total + jnp.where(odd, red[q, rows], red[above, rows])
        mine = pl.ds(8 * t, 8)
        value = (total + sblk[q, mine]) * SIXTH
        if final:
            other = red[q + 1, rows]
            fld[2 * q, mine] = jnp.where(odd, value, other)
            fld[2 * q + 1, mine] = jnp.where(odd, other, value)
        else:
            blk[r + 1, q + 1, rows] = value
            collect(qlo, qhi, (r + 1,), t, q, value)

    def store(q):
        planes = pl.ds(2 * q, 2)
        return pltpu.make_async_copy(fld.at[planes], out.at[planes], store_sem.at[q])

    def sweep(r, final):
        here = functools.partial(message, r)
        each(here, MESSAGES, "arrived", Z_FACES)

        @pl.when(r == 0)
        def _():
            each(smessage, FACES, "arrived", Z_FACES)

        columns(r, False)

        def red_inner(n, c):
            for q in (2 * n + 1, 2 * n + 2):
                for t in range(1, TILES - 1):
                    red_tile(r, q, t)
            return c

        lax.fori_loop(0, 3, red_inner, 0)

        def black_inner(n, c):
            for q in (2 * n, 2 * n + 1):
                for t in range(2, TILES - 2):
                    black_tile(r, q, t, final)
            return c

        lax.fori_loop(1, 3, black_inner, 0)

        rest = [d for d in MESSAGES if d not in Z_FACES]
        each(here, MESSAGES, "arrived", rest)

        @pl.when(r == 0)
        def _():
            each(smessage, FACES, "arrived", [d for d in FACES if d not in Z_FACES])

        each(here, MESSAGES, "sent")
        columns(r, True)
        for q in (0, NQ - 1):
            for t in range(1, TILES - 1):
                red_tile(r, q, t)
        for q in range(NQ):
            for t in (-1, 0, TILES - 1, TILES):
                red_tile(r, q, t)
        halo_tiles(r)
        for q in range(2, 6):
            for t in (0, 1, TILES - 2, TILES - 1):
                black_tile(r, q, t, final)
            if final:
                store(q).start()
        for q in (0, 1, 6, 7):
            for t in range(TILES):
                black_tile(r, q, t, final)
            if final:
                store(q).start()
        if not final:
            settle(qlo, (r + 1,))
            each(functools.partial(message, r + 1), MESSAGES, "start")

    def sweeps(r, c):
        sweep(r, False)
        return c

    lax.fori_loop(0, SWEEPS - 1, sweeps, 0)
    sweep(SWEEPS - 1, True)
    each(smessage, FACES, "sent")
    for q in range(NQ):
        store(q).wait()


def on_device(field, source):
    f32 = jnp.float32
    dma = pltpu.SemaphoreType.DMA
    columns = pltpu.VMEM((COLS, NZ), f32)
    return pl.pallas_call(
        kernel,
        name="smooth",
        out_shape=jax.ShapeDtypeStruct(field.shape, f32),
        in_specs=[pl.BlockSpec(memory_space=pl.ANY)] * 2,
        out_specs=pl.BlockSpec(memory_space=pl.ANY),
        scratch_shapes=[
            pltpu.VMEM((2 * NQ, NY, NZ), f32),
            pltpu.VMEM((2 * NQ, NY, NZ), f32),
            pltpu.VMEM((SWEEPS, NQ + 2, ROWS, NZ), f32),
            pltpu.VMEM((NQ + 1, ROWS, NZ), f32),
            pltpu.VMEM((NQ + 2, ROWS, NZ), f32),
            pltpu.VMEM((NQ, NY, NZ), f32),
            pltpu.VMEM((SWEEPS, 3, COLS + 16, NZ), f32),
            pltpu.VMEM((SWEEPS, 3, COLS + 16, NZ), f32),
            pltpu.VMEM((SWEEPS, COLS, NZ), f32),
            pltpu.VMEM((SWEEPS, COLS, NZ), f32),
            columns, columns, columns, columns,
            pltpu.VMEM((COLS + 16, NZ), f32),
            columns, columns,
            dma((2, 4)),
            dma((NQ,)),
            dma((len(MESSAGES),)),
            dma((SWEEPS, len(MESSAGES))),
            dma((len(FACES),)),
            dma((len(FACES),)),
        ],
        compiler_params=pltpu.CompilerParams(collective_id=0, has_side_effects=True),
    )(field, source)


def solution(mesh):
    spec = P("gx", "gy", "gz")
    return jax.shard_map(
        on_device, mesh=mesh, in_specs=(spec, spec), out_specs=spec, check_vma=False
    )
```

```python
import functools
import itertools

import jax
import jax.numpy as jnp
from jax import lax
from jax.experimental import pallas as pl
from jax.experimental.pallas import tpu as pltpu
from jax.sharding import PartitionSpec as P

MESH = pl.DeviceIdType.MESH
SWEEPS = 3
NQ, NY, NZ = 8, 256, 128
TILES = NY // 8
TOP = 16
ROWS = NY + 2 * TOP
VECS = TILES // 8
COLS = 8 * VECS
SIXTH = 1.0 / 6.0

EDGES = [d for d in itertools.product((-1, 0, 1), repeat=3) if sum(map(abs, d)) == 2]
FACES = [(0, 0, 1), (0, 0, -1), (0, 1, 0), (0, -1, 0), (1, 0, 0), (-1, 0, 0)]
MESSAGES = [d for d in EDGES if d[0] == 0] + [d for d in EDGES if d[0]] + FACES
Z_FACES = [(0, 0, 1), (0, 0, -1)]


def when(cond, f):
    if cond is None:
        f()
    else:
        pl.when(cond)(f)


def kernel(
    field, source, red, black,
    fld, src, blk, sred, sblk, ql, qr, qlo, qhi, sql, sqr, sqlo, sqhi, ins, xins, rins,
    load_sem, send_sem, recv_sem, ssend_sem, srecv_sem,
):
    gx, gy, gz = (lax.axis_index(a) for a in ("gx", "gy", "gz"))
    nx, ny, nz = (lax.axis_size(a) for a in ("gx", "gy", "gz"))
    low_wall, high_wall = gx == 0, gx == nx - 1

    def device(d):
        return {
            "gx": gx + d[0],
            "gy": lax.rem(gy + d[1] + ny, ny),
            "gz": lax.rem(gz + d[2] + nz, nz),
        }

    def exists(d):
        if d[0] > 0:
            return gx < nx - 1
        if d[0] < 0:
            return gx > 0
        return None

    def opposite(d):
        return tuple(-v for v in d)

    def block_slices(d):
        dx, dy, _ = d
        sp, dp = ((8, 0) if dx > 0 else (1, 9)) if dx else (pl.ds(1, NQ), pl.ds(1, NQ))
        sr, dr = ((TOP + NY - 8, TOP - 8) if dy > 0 else (TOP, TOP + NY)) if dy else (TOP, TOP)
        n = 8 if dy else NY
        return (sp, pl.ds(sr, n)), (dp, pl.ds(dr, n))

    def refs(r, d):
        dx, dy, dz = d
        if dz == 0:
            s, t = block_slices(d)
            return blk.at[(r, *s)], blk.at[(r, *t)]
        col, dst = (qhi, ql) if dz > 0 else (qlo, qr)
        own = pl.ds(8, COLS)
        if dx:
            return col.at[r], dst.at[r, 0 if dx > 0 else 2, own]
        if dy:
            sr, dr = (COLS - 8, 0) if dy > 0 else (0, COLS + 8)
            return col.at[r, pl.ds(sr, 8)], dst.at[r, 1, pl.ds(dr, 8)]
        return col.at[r], dst.at[r, 1, own]

    def message(r, m):
        d = MESSAGES[m]
        s, t = refs(r, d)
        return pltpu.make_async_remote_copy(
            src_ref=s, dst_ref=t, send_sem=send_sem.at[m], recv_sem=recv_sem.at[r, m],
            device_id=device(d), device_id_type=MESH,
        )

    def smessage(m):
        d = FACES[m]
        if d[2]:
            s, t = (sqhi, sql) if d[2] > 0 else (sqlo, sqr)
        else:
            s, t = block_slices(d)
            s, t = sred.at[s], sred.at[t]
        return pltpu.make_async_remote_copy(
            src_ref=s, dst_ref=t, send_sem=ssend_sem.at[m], recv_sem=srecv_sem.at[m],
            device_id=device(d), device_id_type=MESH,
        )

    def each(make, dirs, what, select=None):
        for m, d in enumerate(dirs):
            if select is not None and d not in select:
                continue
            if what == "start":
                when(exists(d), lambda m=m: make(m).start())
            elif what == "sent":
                when(exists(d), lambda m=m: make(m).wait_send())
            else:
                when(exists(opposite(d)), lambda m=m: make(m).wait_recv())

    barrier = pltpu.get_barrier_semaphore()
    for d in MESSAGES:
        when(exists(d), lambda d=d: pl.semaphore_signal(barrier, inc=1, device_id=device(d), device_id_type=MESH))

    def load(array, buffer, half, n):
        planes = pl.ds(4 * n, 4)
        return pltpu.make_async_copy(array.at[planes], buffer.at[planes], load_sem.at[half, n])

    for n in range(4):
        load(field, fld, 0, n).start()
    for n in range(4):
        load(source, src, 1, n).start()

    lane = lax.broadcasted_iota(jnp.int32, (8, NZ), 1)
    sub = lax.broadcasted_iota(jnp.int32, (8, NZ), 0)
    odd = jnp.bitwise_and(lane + sub, 1) == 1
    even_lane = jnp.bitwise_and(lane, 1) == 0
    first, last = lane == 0, lane == NZ - 1
    group = jnp.bitwise_and(lane, 15)
    half = jnp.right_shift(lane, 1)
    half_after = jnp.bitwise_and(half - 1, NZ // 2 - 1)

    def roll(x, shift):
        return pltpu.roll(x, shift, 1)

    def slot(t, q):
        return 8 * (t % 8) + q

    def collect(lo, hi, lead, t, q, value):
        m = slot(t, q)
        turned = roll(value, jnp.bitwise_and(2 * m + 2, NZ - 1))
        rows = pl.ds(8 * (t // 8), 8)
        hi[(*lead, rows)] = jnp.where(half == m, turned, hi[(*lead, rows)])
        lo[(*lead, rows)] = jnp.where(half_after == m, turned, lo[(*lead, rows)])

    def settle(lo, lead):
        for v in range(VECS):
            rows = pl.ds(8 * v, 8)
            lo[(*lead, rows)] = roll(lo[(*lead, rows)], NZ - 2)

    zero = jnp.zeros((ROWS, NZ), jnp.float32)

    def wall(pair, plane):
        for r in range(SWEEPS):
            blk[r, pair] = zero
            ql[r, plane] = jnp.zeros((COLS + 16, NZ), jnp.float32)
            qr[r, plane] = jnp.zeros((COLS + 16, NZ), jnp.float32)
        sred[pair] = zero

    pl.when(low_wall)(lambda: wall(0, 0))
    pl.when(high_wall)(lambda: wall(9, 2))
    inside = jnp.where(odd, jnp.where(low_wall, 0.0, SIXTH), jnp.where(high_wall, 0.0, SIXTH))

    def pack_field(q, c):
        for t in range(TILES):
            rows = pl.ds(8 * t, 8)
            value = jnp.where(odd, fld[2 * q, rows], fld[2 * q + 1, rows])
            blk[0, q + 1, pl.ds(TOP + 8 * t, 8)] = value
            collect(qlo, qhi, (0,), t, q, value)
        return c

    for n in range(4):
        load(field, fld, 0, n).wait()
        lax.fori_loop(2 * n, 2 * n + 2, pack_field, 0)
    settle(qlo, (0,))

    walls = jnp.where(jnp.logical_or(low_wall, high_wall), 1, 0)
    pl.semaphore_wait(barrier, len(MESSAGES) - 5 * walls)
    each(functools.partial(message, 0), MESSAGES, "start")

    def pack_source(q, c):
        for t in range(TILES):
            rows = pl.ds(8 * t, 8)
            even_plane, odd_plane = src[2 * q, rows], src[2 * q + 1, rows]
            value = jnp.where(odd, odd_plane, even_plane)
            sred[q + 1, pl.ds(TOP + 8 * t, 8)] = value
            sblk[q, rows] = jnp.where(odd, even_plane, odd_plane)
            collect(sqlo, sqhi, (), t, q, value)
        return c

    for n in range(4):
        load(source, src, 1, n).wait()
        lax.fori_loop(2 * n, 2 * n + 2, pack_source, 0)
    settle(sqlo, ())
    each(smessage, FACES, "start")

    def columns(r, edges):
        for v in range(-1, VECS + 1) if edges else range(VECS):
            rows = pl.ds(8 * v + 8, 8)
            ins[rows] = jnp.where(even_lane, qr[r, 1, rows], ql[r, 1, rows])
        for v in range(VECS):
            here, rows = pl.ds(8 * v + 8, 8), pl.ds(8 * v, 8)
            c = ins[here]
            before = ins[rows] if edges or v > 0 else c
            after = ins[pl.ds(8 * v + 16, 8)] if edges or v < VECS - 1 else c
            back = roll(jnp.where(lane >= NZ - 16, before, c), 16)
            ahead = roll(jnp.where(lane < 16, after, c), NZ - 16)
            total = c + jnp.where(sub == 0, pltpu.roll(back, 1, 0), pltpu.roll(c, 1, 0))
            total = total + jnp.where(sub == 7, pltpu.roll(ahead, 7, 0), pltpu.roll(c, 7, 0))
            up, down = roll(c, NZ - 2), roll(c, 2)
            if edges:
                above = jnp.where(even_lane, qr[r, 2, here], ql[r, 2, here])
                below = jnp.where(even_lane, qr[r, 0, here], ql[r, 0, here])
                up = jnp.where(group >= 14, roll(above, 14), up)
                down = jnp.where(group < 2, roll(below, NZ - 14), down)
                xins[rows] = jnp.where(odd, above, roll(below, NZ - 14))
            total = total + jnp.where(odd, up, down)
            left, right = ql[r, 1, here] + qlo[r, rows], qr[r, 1, here] + qhi[r, rows]
            total = total + jnp.where(even_lane, roll(right, NZ - 1), roll(left, 1))
            total = total + jnp.where(even_lane, sqr[rows], sql[rows])
            rins[rows] = total * SIXTH

    def beside(c, edge, m):
        edge = roll(edge, NZ - 1 - 2 * m)
        return jnp.where(first, edge, roll(c, 1)) + jnp.where(last, edge, roll(c, NZ - 1))

    def around(ref, lead, row, edge, m):
        c = ref[(*lead, pl.ds(row, 8))]
        total = c + ref[(*lead, pl.ds(row - 1, 8))] + ref[(*lead, pl.ds(row + 1, 8))]
        return total + beside(c, edge, m)

    def red_tile(r, q, t):
        rows = pl.ds(TOP + 8 * t, 8)
        total = around(blk, (r, q + 1), TOP + 8 * t, ins[pl.ds(8 * (t // 8) + 8, 8)], slot(t, q))
        total = total + jnp.where(odd, blk[r, q + 2, rows], blk[r, q, rows])
        red[q + 1, rows] = (total + sred[q + 1, rows]) * SIXTH

    def halo_tiles(r):
        for t in range(TILES):
            row = TOP + 8 * t
            rows = pl.ds(row, 8)
            low, high = blk[r, 0, rows], blk[r, 9, rows]
            c, far = jnp.where(odd, high, low), jnp.where(odd, low, high)
            total = jnp.where(odd, blk[r, 0, pl.ds(row - 1, 8)], blk[r, 9, pl.ds(row - 1, 8)])
            total = total + jnp.where(odd, blk[r, 0, pl.ds(row + 1, 8)], blk[r, 9, pl.ds(row + 1, 8)])
            total = total + beside(c, xins[pl.ds(8 * (t // 8), 8)], slot(t, 0))
            total = total + far + jnp.where(odd, blk[r, 1, rows], blk[r, 8, rows])
            total = total + jnp.where(odd, sred[0, rows], sred[9, rows])
            red[0, rows] = total * inside

    def black_tile(r, q, t, final):
        rows = pl.ds(TOP + 8 * t, 8)
        total = around(red, (q + 1,), TOP + 8 * t, rins[pl.ds(8 * (t // 8), 8)], slot(t, q))
        above = (0 if q == NQ - 1 else q + 2) if isinstance(q, int) else q + 2
        total = total + jnp.where(odd, red[q, rows], red[above, rows])
        mine = pl.ds(8 * t, 8)
        value = (total + sblk[q, mine]) * SIXTH
        if final:
            black[q, mine] = value
        else:
            blk[r + 1, q + 1, rows] = value

    def collect_pair(r, q, tiles):
        for t in tiles:
            collect(qlo, qhi, (r,), t, q, blk[r, q + 1, pl.ds(TOP + 8 * t, 8)])

    def sweep(r, final):
        here = functools.partial(message, r)
        each(here, MESSAGES, "arrived", Z_FACES)

        @pl.when(r == 0)
        def _():
            each(smessage, FACES, "arrived", Z_FACES)

        columns(r, False)

        def red_inner(n, c):
            for q in (2 * n + 1, 2 * n + 2):
                for t in range(1, TILES - 1):
                    red_tile(r, q, t)
            return c

        lax.fori_loop(0, 3, red_inner, 0)

        def black_inner(n, c):
            for q in (2 * n, 2 * n + 1):
                for t in range(2, TILES - 2):
                    black_tile(r, q, t, final)
            return c

        lax.fori_loop(1, 3, black_inner, 0)

        def collect_inner(q, c):
            collect_pair(r + 1, q, range(2, TILES - 2))
            return c

        if not final:
            lax.fori_loop(2, 6, collect_inner, 0)

        rest = [d for d in MESSAGES if d not in Z_FACES]
        each(here, MESSAGES, "arrived", rest)

        @pl.when(r == 0)
        def _():
            each(smessage, FACES, "arrived", [d for d in FACES if d not in Z_FACES])

        each(here, MESSAGES, "sent")
        columns(r, True)
        for q in (0, NQ - 1):
            for t in range(1, TILES - 1):
                red_tile(r, q, t)
        for q in range(NQ):
            for t in (-1, 0, TILES - 1, TILES):
                red_tile(r, q, t)
        halo_tiles(r)
        for q in range(2, 6):
            for t in (0, 1, TILES - 2, TILES - 1):
                black_tile(r, q, t, final)
        for q in (0, 1, 6, 7):
            for t in range(TILES):
                black_tile(r, q, t, final)
        if not final:
            for q in range(2, 6):
                collect_pair(r + 1, q, (0, 1, TILES - 2, TILES - 1))

            def collect_outer(n, c):
                collect_pair(r + 1, n + jnp.where(n >= 2, 4, 0), range(TILES))
                return c

            lax.fori_loop(0, 4, collect_outer, 0)
            settle(qlo, (r + 1,))
            each(functools.partial(message, r + 1), MESSAGES, "start")

    def sweeps(r, c):
        sweep(r, False)
        return c

    lax.fori_loop(0, SWEEPS - 1, sweeps, 0)
    sweep(SWEEPS - 1, True)
    each(smessage, FACES, "sent")


def unpack(red, black, out, buf, sem):
    sub = lax.broadcasted_iota(jnp.int32, (8, NZ), 0)
    odd = jnp.bitwise_and(lax.broadcasted_iota(jnp.int32, (8, NZ), 1) + sub, 1) == 1

    def store(q):
        planes = pl.ds(2 * q, 2)
        return pltpu.make_async_copy(buf.at[planes], out.at[planes], sem.at[q])

    def merge(q, c):
        for t in range(TILES):
            rows = pl.ds(8 * t, 8)
            x, y = red[q + 1, pl.ds(TOP + 8 * t, 8)], black[q, rows]
            buf[2 * q, rows] = jnp.where(odd, y, x)
            buf[2 * q + 1, rows] = jnp.where(odd, x, y)
        store(q).start()
        return c

    lax.fori_loop(0, NQ, merge, 0)

    def stored(q, c):
        store(q).wait()
        return c

    lax.fori_loop(0, NQ, stored, 0)


def on_device(field, source):
    f32 = jnp.float32
    dma = pltpu.SemaphoreType.DMA
    columns = pltpu.VMEM((COLS, NZ), f32)
    vmem = pl.BlockSpec(memory_space=pltpu.VMEM)
    red, black = pl.pallas_call(
        kernel,
        name="smooth",
        out_shape=(pltpu.VMEM((NQ + 1, ROWS, NZ), f32), pltpu.VMEM((NQ, NY, NZ), f32)),
        in_specs=[pl.BlockSpec(memory_space=pl.ANY)] * 2,
        out_specs=(vmem, vmem),
        scratch_shapes=[
            pltpu.VMEM((2 * NQ, NY, NZ), f32),
            pltpu.VMEM((2 * NQ, NY, NZ), f32),
            pltpu.VMEM((SWEEPS, NQ + 2, ROWS, NZ), f32),
            pltpu.VMEM((NQ + 2, ROWS, NZ), f32),
            pltpu.VMEM((NQ, NY, NZ), f32),
            pltpu.VMEM((SWEEPS, 3, COLS + 16, NZ), f32),
            pltpu.VMEM((SWEEPS, 3, COLS + 16, NZ), f32),
            pltpu.VMEM((SWEEPS, COLS, NZ), f32),
            pltpu.VMEM((SWEEPS, COLS, NZ), f32),
            columns, columns, columns, columns,
            pltpu.VMEM((COLS + 16, NZ), f32),
            columns, columns,
            dma((2, 4)),
            dma((len(MESSAGES),)),
            dma((SWEEPS, len(MESSAGES))),
            dma((len(FACES),)),
            dma((len(FACES),)),
        ],
        compiler_params=pltpu.CompilerParams(collective_id=0, has_side_effects=True),
    )(field, source)
    red, black = (pltpu.with_memory_space_constraint(x, pltpu.VMEM) for x in (red, black))
    return pl.pallas_call(
        unpack,
        name="unpack",
        out_shape=jax.ShapeDtypeStruct(field.shape, f32),
        in_specs=[vmem, vmem],
        out_specs=pl.BlockSpec(memory_space=pl.ANY),
        scratch_shapes=[pltpu.VMEM((2 * NQ, NY, NZ), f32), dma((NQ,))],
    )(red, black)


def solution(mesh):
    spec = P("gx", "gy", "gz")
    return jax.shard_map(
        on_device, mesh=mesh, in_specs=(spec, spec), out_specs=spec, check_vma=False
    )
```

```python
import functools
import itertools

import jax
import jax.numpy as jnp
from jax import lax
from jax.experimental import pallas as pl
from jax.experimental.pallas import tpu as pltpu
from jax.sharding import PartitionSpec as P

MESH = pl.DeviceIdType.MESH
SWEEPS = 3
NQ, NY, NZ = 8, 256, 128
TILES = NY // 8
ENDS = (0, TILES - 1)
TOP = 16
ROWS = NY + 2 * TOP
VECS = TILES // 8
COLS = 8 * VECS
SIXTH = 1.0 / 6.0

EDGES = [d for d in itertools.product((-1, 0, 1), repeat=3) if sum(map(abs, d)) == 2]
FACES = [(0, 0, 1), (0, 0, -1), (0, 1, 0), (0, -1, 0), (1, 0, 0), (-1, 0, 0)]
MESSAGES = [d for d in EDGES if d[0] == 0] + [d for d in EDGES if d[0]] + FACES
X_FACES, Y_FACES, Z_FACES = FACES[4:], FACES[2:4], FACES[:2]
YZ_EDGES, XY_EDGES, XZ_EDGES = ([d for d in EDGES if d[a] == 0] for a in (0, 2, 1))


def when(cond, f):
    if cond is None:
        f()
    else:
        pl.when(cond)(f)


def kernel(
    field, source, red, black,
    fld, src, blk, sred, sblk, ql, qr, qlo, qhi, elo, ehi, sql, sqr, sqlo, sqhi, ins, xins, rins, sxs, sxd, sx,
    load_sem, send_sem, recv_sem, ssend_sem, srecv_sem,
):
    def load(array, buffer, half, n):
        planes = pl.ds(2 * n, 2)
        return pltpu.make_async_copy(array.at[planes], buffer.at[planes], load_sem.at[half, n])

    for n in range(NQ):
        load(field, fld, 0, n).start()

    gx, gy, gz = (lax.axis_index(a) for a in ("gx", "gy", "gz"))
    nx, ny, nz = (lax.axis_size(a) for a in ("gx", "gy", "gz"))
    low_wall, high_wall = gx == 0, gx == nx - 1

    def device(d):
        return {
            "gx": gx + d[0],
            "gy": lax.rem(gy + d[1] + ny, ny),
            "gz": lax.rem(gz + d[2] + nz, nz),
        }

    def exists(d):
        if d[0] > 0:
            return gx < nx - 1
        if d[0] < 0:
            return gx > 0
        return None

    def opposite(d):
        return tuple(-v for v in d)

    def block_slices(d):
        dx, dy, _ = d
        sp, dp = ((8, 0) if dx > 0 else (1, 9)) if dx else (pl.ds(1, NQ), pl.ds(1, NQ))
        sr, dr = ((TOP + NY - 8, TOP - 8) if dy > 0 else (TOP, TOP + NY)) if dy else (TOP, TOP)
        n = 8 if dy else NY
        return (sp, pl.ds(sr, n)), (dp, pl.ds(dr, n))

    def refs(r, d):
        dx, dy, dz = d
        if dz == 0:
            s, t = block_slices(d)
            return blk.at[(r, *s)], blk.at[(r, *t)]
        col, dst = (qhi, ql) if dz > 0 else (qlo, qr)
        own = pl.ds(8, COLS)
        if dx:
            return col.at[r], dst.at[r, 0 if dx > 0 else 2, own]
        if dy:
            end, dr = (1, 0) if dy > 0 else (0, COLS + 8)
            return (ehi if dz > 0 else elo).at[r, end], dst.at[r, 1, pl.ds(dr, 8)]
        return col.at[r], dst.at[r, 1, own]

    def message(r, m):
        d = MESSAGES[m]
        s, t = refs(r, d)
        return pltpu.make_async_remote_copy(
            src_ref=s, dst_ref=t, send_sem=send_sem.at[m], recv_sem=recv_sem.at[r, m],
            device_id=device(d), device_id_type=MESH,
        )

    def smessage(m):
        d = FACES[m]
        if d[2]:
            s, t = (sqhi, sql) if d[2] > 0 else (sqlo, sqr)
        elif d[0]:
            side = 0 if d[0] > 0 else 1
            s, t = sxs.at[side], sxd.at[side]
        else:
            s, t = block_slices(d)
            s, t = sred.at[s], sred.at[t]
        return pltpu.make_async_remote_copy(
            src_ref=s, dst_ref=t, send_sem=ssend_sem.at[m], recv_sem=srecv_sem.at[m],
            device_id=device(d), device_id_type=MESH,
        )

    def each(make, dirs, what, select=None):
        for m, d in enumerate(dirs):
            if select is not None and d not in select:
                continue
            if what == "start":
                when(exists(d), lambda m=m: make(m).start())
            elif what == "sent":
                when(exists(d), lambda m=m: make(m).wait_send())
            else:
                when(exists(opposite(d)), lambda m=m: make(m).wait_recv())

    barrier = pltpu.get_barrier_semaphore()
    for d in MESSAGES:
        when(exists(d), lambda d=d: pl.semaphore_signal(barrier, inc=1, device_id=device(d), device_id_type=MESH))

    lane = lax.broadcasted_iota(jnp.int32, (8, NZ), 1)
    sub = lax.broadcasted_iota(jnp.int32, (8, NZ), 0)
    odd = jnp.bitwise_and(lane + sub, 1) == 1
    even_lane = jnp.bitwise_and(lane, 1) == 0
    first, last = lane == 0, lane == NZ - 1
    outer = jnp.logical_or(first, last)
    group = jnp.bitwise_and(lane, 15)
    half = jnp.right_shift(lane, 1)
    half_after = jnp.bitwise_and(half - 1, NZ // 2 - 1)

    def roll(x, shift):
        return pltpu.roll(x, shift, 1)

    def slot(t, q):
        return 8 * (t % 8) + q

    def collect(lo, hi, lead, t, q, value, rows=None):
        m = slot(t, q)
        turned = roll(value, jnp.bitwise_and(2 * m + 2, NZ - 1))
        rows = pl.ds(8 * (t // 8), 8) if rows is None else rows
        hi[(*lead, rows)] = jnp.where(half == m, turned, hi[(*lead, rows)])
        lo[(*lead, rows)] = jnp.where(half_after == m, turned, lo[(*lead, rows)])

    def collect_edges(r):
        for end, t in enumerate(ENDS):
            for q in range(NQ):
                collect(elo, ehi, (r, end), t, q, blk[r, q + 1, pl.ds(TOP + 8 * t, 8)], pl.ds(0, 8))
            elo[r, end] = roll(elo[r, end], NZ - 2)

    def settle(lo, lead):
        for v in range(VECS):
            rows = pl.ds(8 * v, 8)
            lo[(*lead, rows)] = roll(lo[(*lead, rows)], NZ - 2)

    zero = jnp.zeros((ROWS, NZ), jnp.float32)

    def wall(pair, plane):
        for r in range(SWEEPS):
            blk[r, pair] = zero
            ql[r, plane] = jnp.zeros((COLS + 16, NZ), jnp.float32)
            qr[r, plane] = jnp.zeros((COLS + 16, NZ), jnp.float32)
        sxd[0 if pair == 0 else 1] = jnp.zeros((NY // 2, NZ), jnp.float32)

    pl.when(low_wall)(lambda: wall(0, 0))
    pl.when(high_wall)(lambda: wall(9, 2))
    inside = jnp.where(odd, jnp.where(low_wall, 0.0, SIXTH), jnp.where(high_wall, 0.0, SIXTH))

    def pack_field(q, c):
        for t in range(TILES):
            rows = pl.ds(8 * t, 8)
            value = jnp.where(odd, fld[2 * q, rows], fld[2 * q + 1, rows])
            blk[0, q + 1, pl.ds(TOP + 8 * t, 8)] = value
            collect(qlo, qhi, (0,), t, q, value)
        return c

    def packed_field(q, c):
        load(field, fld, 0, q).wait()
        load(source, src, 1, q).start()
        return pack_field(q, c)

    lax.fori_loop(0, NQ, packed_field, 0)
    collect_edges(0)
    settle(qlo, (0,))

    walls = jnp.where(jnp.logical_or(low_wall, high_wall), 1, 0)
    pl.semaphore_wait(barrier, len(MESSAGES) - 5 * walls)
    each(functools.partial(message, 0), MESSAGES, "start")

    def pack_source(q, c):
        for t in range(TILES):
            rows = pl.ds(8 * t, 8)
            even_plane, odd_plane = src[2 * q, rows], src[2 * q + 1, rows]
            value = jnp.where(odd, odd_plane, even_plane)
            sred[q + 1, pl.ds(TOP + 8 * t, 8)] = value
            sblk[q, rows] = jnp.where(odd, even_plane, odd_plane)
            collect(sqlo, sqhi, (), t, q, value)
        return c

    def packed_source(q, c):
        load(source, src, 1, q).wait()
        return pack_source(q, c)

    def swap(x):
        return jnp.where(jnp.bitwise_and(sub, 1) == 0, pltpu.roll(x, 7, 0), pltpu.roll(x, 1, 0))

    lax.fori_loop(0, NQ, packed_source, 0)
    settle(sqlo, ())
    each(smessage, FACES, "start", Z_FACES + Y_FACES)
    for t in range(TILES // 2):
        near, away = pl.ds(TOP + 8 * t, 8), pl.ds(TOP + 8 * t + NY // 2, 8)
        sxs[0, pl.ds(8 * t, 8)] = jnp.where(odd, sred[NQ, near], swap(sred[NQ, away]))
        sxs[1, pl.ds(8 * t, 8)] = jnp.where(odd, swap(sred[1, away]), sred[1, near])
    each(smessage, FACES, "start", X_FACES)

    def columns(r, edges):
        for v in range(-1, VECS + 1) if edges else range(VECS):
            rows = pl.ds(8 * v + 8, 8)
            ins[rows] = jnp.where(even_lane, qr[r, 1, rows], ql[r, 1, rows])
        for v in range(VECS):
            here, rows = pl.ds(8 * v + 8, 8), pl.ds(8 * v, 8)
            c = ins[here]
            before = ins[rows] if edges or v > 0 else c
            after = ins[pl.ds(8 * v + 16, 8)] if edges or v < VECS - 1 else c
            back = roll(jnp.where(lane >= NZ - 16, before, c), 16)
            ahead = roll(jnp.where(lane < 16, after, c), NZ - 16)
            total = c + jnp.where(sub == 0, pltpu.roll(back, 1, 0), pltpu.roll(c, 1, 0))
            total = total + jnp.where(sub == 7, pltpu.roll(ahead, 7, 0), pltpu.roll(c, 7, 0))
            up, down = roll(c, NZ - 2), roll(c, 2)
            if edges:
                above = jnp.where(even_lane, qr[r, 2, here], ql[r, 2, here])
                below = jnp.where(even_lane, qr[r, 0, here], ql[r, 0, here])
                up = jnp.where(group >= 14, roll(above, 14), up)
                down = jnp.where(group < 2, roll(below, NZ - 14), down)
                xins[rows] = jnp.where(odd, above, roll(below, NZ - 14))
            total = total + jnp.where(odd, up, down)
            left, right = ql[r, 1, here] + qlo[r, rows], qr[r, 1, here] + qhi[r, rows]
            total = total + jnp.where(even_lane, roll(right, NZ - 1), roll(left, 1))
            total = total + jnp.where(even_lane, sqr[rows], sql[rows])
            rins[rows] = total * SIXTH

    def beside(c, edge, m):
        edge = roll(edge, NZ - 1 - 2 * m)
        return jnp.where(first, edge, roll(c, 1)) + jnp.where(last, edge, roll(c, NZ - 1))

    def around(ref, lead, row, edge, m):
        c = ref[(*lead, pl.ds(row, 8))]
        total = c + ref[(*lead, pl.ds(row - 1, 8))] + ref[(*lead, pl.ds(row + 1, 8))]
        return total + beside(c, edge, m)

    def red_tile(r, q, t):
        row = TOP + 8 * t
        rows = pl.ds(row, 8)
        c = blk[r, q + 1, rows]
        total = c + jnp.where(first, 0.0, roll(c, 1)) + jnp.where(last, 0.0, roll(c, NZ - 1))
        up = jnp.where(sub == 0, 0.0, pltpu.roll(c, 1, 0)) if t == 0 else blk[r, q + 1, pl.ds(row - 1, 8)]
        down = jnp.where(sub == 7, 0.0, pltpu.roll(c, 7, 0)) if t == TILES - 1 else blk[r, q + 1, pl.ds(row + 1, 8)]
        above = blk[r, q + 2, rows] if q < NQ - 1 else 0.0
        below = blk[r, q, rows] if q > 0 else 0.0
        total = total + up + down + jnp.where(odd, above, below)
        red[q + 1, rows] = (total + sred[q + 1, rows]) * SIXTH

    def complete_z(q, t):
        rows = pl.ds(TOP + 8 * t, 8)
        edge = roll(ins[pl.ds(8 * (t // 8) + 8, 8)], NZ - 1 - 2 * slot(t, q))
        red[q + 1, rows] = red[q + 1, rows] + jnp.where(outer, edge, 0.0) * SIXTH

    def red_beyond(r, q, t):
        rows = pl.ds(TOP + 8 * t, 8)
        total = around(blk, (r, q + 1), TOP + 8 * t, ins[pl.ds(8 * (t // 8) + 8, 8)], slot(t, q))
        total = total + jnp.where(odd, blk[r, q + 2, rows], blk[r, q, rows])
        red[q + 1, rows] = (total + sred[q + 1, rows]) * SIXTH

    def complete(r, q, t):
        row = TOP + 8 * t
        rows = pl.ds(row, 8)
        more = None
        if t == 0:
            more = jnp.where(sub == 0, blk[r, q + 1, pl.ds(row - 1, 8)], 0.0)
        if t == TILES - 1:
            more = jnp.where(sub == 7, blk[r, q + 1, pl.ds(row + 1, 8)], 0.0)
        side = None
        if q == 0:
            side = jnp.where(odd, 0.0, blk[r, 0, rows])
        if q == NQ - 1:
            side = jnp.where(odd, blk[r, 9, rows], 0.0)
        if side is not None:
            more = side if more is None else more + side
        if more is not None:
            red[q + 1, rows] = red[q + 1, rows] + more * SIXTH

    def halo_tiles(r, tiles):
        for t in tiles:
            row = TOP + 8 * t
            rows = pl.ds(row, 8)
            low, high = blk[r, 0, rows], blk[r, 9, rows]
            c, far = jnp.where(odd, high, low), jnp.where(odd, low, high)
            total = jnp.where(odd, blk[r, 0, pl.ds(row - 1, 8)], blk[r, 9, pl.ds(row - 1, 8)])
            total = total + jnp.where(odd, blk[r, 0, pl.ds(row + 1, 8)], blk[r, 9, pl.ds(row + 1, 8)])
            total = total + beside(c, xins[pl.ds(8 * (t // 8), 8)], slot(t, 0))
            total = total + far + jnp.where(odd, blk[r, 1, rows], blk[r, 8, rows])
            red[0, rows] = (total + sx[pl.ds(8 * t, 8)]) * inside

    def black_tile(r, q, t, final):
        rows = pl.ds(TOP + 8 * t, 8)
        total = around(red, (q + 1,), TOP + 8 * t, rins[pl.ds(8 * (t // 8), 8)], slot(t, q))
        above = (0 if q == NQ - 1 else q + 2) if isinstance(q, int) else q + 2
        total = total + jnp.where(odd, red[q, rows], red[above, rows])
        mine = pl.ds(8 * t, 8)
        value = (total + sblk[q, mine]) * SIXTH
        if final:
            black[q, mine] = value
        else:
            blk[r + 1, q + 1, rows] = value

    def sweep(r, final):
        here = functools.partial(message, r)
        for q in range(NQ):
            for t in range(TILES):
                red_tile(r, q, t)
        each(here, MESSAGES, "arrived", Z_FACES)

        @pl.when(r == 0)
        def _():
            each(smessage, FACES, "arrived", Z_FACES)

        columns(r, False)

        for q in range(NQ):
            for t in range(TILES):
                complete_z(q, t)

        def black_inner(n, c):
            for q in (3 * n + 1, 3 * n + 2, 3 * n + 3):
                for t in range(1, TILES - 1):
                    black_tile(r, q, t, final)
            return c

        lax.fori_loop(0, 2, black_inner, 0)
        if not final:
            for t in range(1, TILES - 1):
                for q in range(1, NQ - 1):
                    collect(qlo, qhi, (r + 1,), t, q, blk[r + 1, q + 1, pl.ds(TOP + 8 * t, 8)])

        rest = [d for d in MESSAGES if d not in Z_FACES]
        each(here, MESSAGES, "arrived", rest)

        @pl.when(r == 0)
        def _():
            each(smessage, FACES, "arrived", [d for d in FACES if d not in Z_FACES])
            for t in range(TILES // 2):
                low, high = sxd[0, pl.ds(8 * t, 8)], sxd[1, pl.ds(8 * t, 8)]
                sx[pl.ds(8 * t, 8)] = jnp.where(odd, low, high)
                sx[pl.ds(8 * t + NY // 2, 8)] = swap(jnp.where(odd, high, low))

        each(here, MESSAGES, "sent")
        columns(r, True)
        for q in range(NQ):
            for t in (-1, TILES):
                red_beyond(r, q, t)
            for t in (0, 1, TILES - 2, TILES - 1):
                complete(r, q, t)
        halo_tiles(r, (0, 1, TILES - 2, TILES - 1))
        for q in range(NQ):
            for t in ENDS:
                black_tile(r, q, t, final)
        after = functools.partial(message, r + 1)
        if not final:
            collect_edges(r + 1)
            each(after, MESSAGES, "start", YZ_EDGES)
            each(after, MESSAGES, "start", XY_EDGES + Y_FACES)
        for q in (0, NQ - 1):
            for t in range(2, TILES - 2):
                complete(r, q, t)
        halo_tiles(r, range(2, TILES - 2))
        for q in (0, NQ - 1):
            for t in range(1, TILES - 1):
                black_tile(r, q, t, final)
        if not final:
            for t in range(TILES):
                for q in range(NQ) if t in ENDS else (0, NQ - 1):
                    collect(qlo, qhi, (r + 1,), t, q, blk[r + 1, q + 1, pl.ds(TOP + 8 * t, 8)])
            settle(qlo, (r + 1,))
            each(after, MESSAGES, "start", XZ_EDGES + Z_FACES)
            each(after, MESSAGES, "start", X_FACES)

    def sweeps(r, c):
        sweep(r, False)
        return c

    lax.fori_loop(0, SWEEPS - 1, sweeps, 0)
    sweep(SWEEPS - 1, True)
    each(smessage, FACES, "sent")


def unpack(red, black, out, buf, sem):
    sub = lax.broadcasted_iota(jnp.int32, (8, NZ), 0)
    odd = jnp.bitwise_and(lax.broadcasted_iota(jnp.int32, (8, NZ), 1) + sub, 1) == 1

    def store(q):
        planes = pl.ds(2 * q, 2)
        return pltpu.make_async_copy(buf.at[planes], out.at[planes], sem.at[q])

    def merge(q, c):
        for t in range(TILES):
            rows = pl.ds(8 * t, 8)
            x, y = red[q + 1, pl.ds(TOP + 8 * t, 8)], black[q, rows]
            buf[2 * q, rows] = jnp.where(odd, y, x)
            buf[2 * q + 1, rows] = jnp.where(odd, x, y)
        store(q).start()
        return c

    lax.fori_loop(0, NQ, merge, 0)

    def stored(q, c):
        store(q).wait()
        return c

    lax.fori_loop(0, NQ, stored, 0)


def on_device(field, source):
    f32 = jnp.float32
    dma = pltpu.SemaphoreType.DMA
    columns = pltpu.VMEM((COLS, NZ), f32)
    vmem = pl.BlockSpec(memory_space=pltpu.VMEM)
    red, black = pl.pallas_call(
        kernel,
        name="smooth",
        out_shape=(pltpu.VMEM((NQ + 1, ROWS, NZ), f32), pltpu.VMEM((NQ, NY, NZ), f32)),
        in_specs=[pl.BlockSpec(memory_space=pl.ANY)] * 2,
        out_specs=(vmem, vmem),
        scratch_shapes=[
            pltpu.VMEM((2 * NQ, NY, NZ), f32),
            pltpu.VMEM((2 * NQ, NY, NZ), f32),
            pltpu.VMEM((SWEEPS, NQ + 2, ROWS, NZ), f32),
            pltpu.VMEM((NQ + 2, ROWS, NZ), f32),
            pltpu.VMEM((NQ, NY, NZ), f32),
            pltpu.VMEM((SWEEPS, 3, COLS + 16, NZ), f32),
            pltpu.VMEM((SWEEPS, 3, COLS + 16, NZ), f32),
            pltpu.VMEM((SWEEPS, COLS, NZ), f32),
            pltpu.VMEM((SWEEPS, COLS, NZ), f32),
            pltpu.VMEM((SWEEPS, 2, 8, NZ), f32),
            pltpu.VMEM((SWEEPS, 2, 8, NZ), f32),
            columns, columns, columns, columns,
            pltpu.VMEM((COLS + 16, NZ), f32),
            columns, columns,
            pltpu.VMEM((2, NY // 2, NZ), f32),
            pltpu.VMEM((2, NY // 2, NZ), f32),
            pltpu.VMEM((NY, NZ), f32),
            dma((2, NQ)),
            dma((len(MESSAGES),)),
            dma((SWEEPS, len(MESSAGES))),
            dma((len(FACES),)),
            dma((len(FACES),)),
        ],
        compiler_params=pltpu.CompilerParams(collective_id=0, has_side_effects=True),
    )(field, source)
    red, black = (pltpu.with_memory_space_constraint(x, pltpu.VMEM) for x in (red, black))
    return pl.pallas_call(
        unpack,
        name="unpack",
        out_shape=jax.ShapeDtypeStruct(field.shape, f32),
        in_specs=[vmem, vmem],
        out_specs=pl.BlockSpec(memory_space=pl.ANY),
        scratch_shapes=[pltpu.VMEM((2 * NQ, NY, NZ), f32), dma((NQ,))],
    )(red, black)


def solution(mesh):
    spec = P("gx", "gy", "gz")
    return jax.shard_map(
        on_device, mesh=mesh, in_specs=(spec, spec), out_specs=spec, check_vma=False
    )
```

```python
import functools
import itertools
import types

import jax
import jax.numpy as jnp
from jax import lax
from jax.experimental import pallas as pl
from jax.experimental.pallas import tpu as pltpu
from jax.sharding import PartitionSpec as P

MESH = pl.DeviceIdType.MESH
SWEEPS = 3
NQ, NY, NZ = 8, 256, 128
TILES = NY // 8
ENDS = (0, TILES - 1)
TOP = 16
ROWS = NY + 2 * TOP
VECS = TILES // 8
COLS = 8 * VECS
SIXTH = 1.0 / 6.0
VMEM_GRANT = 24 << 20

EDGES = [d for d in itertools.product((-1, 0, 1), repeat=3) if sum(map(abs, d)) == 2]
FACES = [(0, 0, 1), (0, 0, -1), (0, 1, 0), (0, -1, 0), (1, 0, 0), (-1, 0, 0)]
MESSAGES = [d for d in EDGES if d[0] == 0] + [d for d in EDGES if d[0]] + FACES
X_FACES, Y_FACES, Z_FACES = FACES[4:], FACES[2:4], FACES[:2]
YZ_EDGES, XY_EDGES, XZ_EDGES = ([d for d in EDGES if d[a] == 0] for a in (0, 2, 1))


def when(cond, f):
    if cond is None:
        f()
    else:
        pl.when(cond)(f)


def cells(blk, red, sred, sblk, ql, qr, qlo, qhi, sql, sqr, sx, merged, ins, xins, rins):
    gx = lax.axis_index("gx")
    low_wall, high_wall = gx == 0, gx == lax.axis_size("gx") - 1
    lane = lax.broadcasted_iota(jnp.int32, (8, NZ), 1)
    sub = lax.broadcasted_iota(jnp.int32, (8, NZ), 0)
    odd = jnp.bitwise_and(lane + sub, 1) == 1
    even_lane = jnp.bitwise_and(lane, 1) == 0
    first, last = lane == 0, lane == NZ - 1
    outer = jnp.logical_or(first, last)
    group = jnp.bitwise_and(lane, 15)
    half = jnp.right_shift(lane, 1)
    half_after = jnp.bitwise_and(half - 1, NZ // 2 - 1)

    def roll(x, shift):
        return pltpu.roll(x, shift, 1)

    def slot(t, q):
        return 8 * (t % 8) + q

    inside = jnp.where(odd, jnp.where(low_wall, 0.0, SIXTH), jnp.where(high_wall, 0.0, SIXTH))

    def swap(x):
        return jnp.where(jnp.bitwise_and(sub, 1) == 0, pltpu.roll(x, 7, 0), pltpu.roll(x, 1, 0))

    def columns(r, edges):
        for v in range(-1, VECS + 1) if edges else range(VECS):
            rows = pl.ds(8 * v + 8, 8)
            ins[rows] = jnp.where(even_lane, qr[r, 1, rows], ql[r, 1, rows])
        for v in range(VECS):
            here, rows = pl.ds(8 * v + 8, 8), pl.ds(8 * v, 8)
            c = ins[here]
            before = ins[rows] if edges or v > 0 else c
            after = ins[pl.ds(8 * v + 16, 8)] if edges or v < VECS - 1 else c
            back = roll(jnp.where(lane >= NZ - 16, before, c), 16)
            ahead = roll(jnp.where(lane < 16, after, c), NZ - 16)
            total = c + jnp.where(sub == 0, pltpu.roll(back, 1, 0), pltpu.roll(c, 1, 0))
            total = total + jnp.where(sub == 7, pltpu.roll(ahead, 7, 0), pltpu.roll(c, 7, 0))
            up, down = roll(c, NZ - 2), roll(c, 2)
            if edges:
                above = jnp.where(even_lane, qr[r, 2, here], ql[r, 2, here])
                below = jnp.where(even_lane, qr[r, 0, here], ql[r, 0, here])
                up = jnp.where(group >= 14, roll(above, 14), up)
                down = jnp.where(group < 2, roll(below, NZ - 14), down)
                xins[rows] = jnp.where(odd, above, roll(below, NZ - 14))
            total = total + jnp.where(odd, up, down)
            left, right = ql[r, 1, here] + qlo[r, rows], qr[r, 1, here] + qhi[r, rows]
            total = total + jnp.where(even_lane, roll(right, NZ - 1), roll(left, 1))
            total = total + jnp.where(even_lane, sqr[rows], sql[rows])
            rins[rows] = total * SIXTH

    def beside(c, edge, m):
        edge = roll(edge, NZ - 1 - 2 * m)
        return jnp.where(first, edge, roll(c, 1)) + jnp.where(last, edge, roll(c, NZ - 1))

    def around(ref, lead, row, edge, m):
        c = ref[(*lead, pl.ds(row, 8))]
        total = c + ref[(*lead, pl.ds(row - 1, 8))] + ref[(*lead, pl.ds(row + 1, 8))]
        return total + beside(c, edge, m)

    def red_tile(r, q, t):
        row = TOP + 8 * t
        rows = pl.ds(row, 8)
        c = blk[r, q + 1, rows]
        total = c + jnp.where(first, 0.0, roll(c, 1)) + jnp.where(last, 0.0, roll(c, NZ - 1))
        up = jnp.where(sub == 0, 0.0, pltpu.roll(c, 1, 0)) if t == 0 else blk[r, q + 1, pl.ds(row - 1, 8)]
        down = jnp.where(sub == 7, 0.0, pltpu.roll(c, 7, 0)) if t == TILES - 1 else blk[r, q + 1, pl.ds(row + 1, 8)]
        above = blk[r, q + 2, rows] if q < NQ - 1 else 0.0
        below = blk[r, q, rows] if q > 0 else 0.0
        total = total + up + down + jnp.where(odd, above, below)
        red[q + 1, rows] = (total + sred[q + 1, rows]) * SIXTH

    def complete_z(q, t):
        rows = pl.ds(TOP + 8 * t, 8)
        edge = roll(ins[pl.ds(8 * (t // 8) + 8, 8)], NZ - 1 - 2 * slot(t, q))
        red[q + 1, rows] = red[q + 1, rows] + jnp.where(outer, edge, 0.0) * SIXTH

    def red_beyond(r, q, t):
        rows = pl.ds(TOP + 8 * t, 8)
        total = around(blk, (r, q + 1), TOP + 8 * t, ins[pl.ds(8 * (t // 8) + 8, 8)], slot(t, q))
        total = total + jnp.where(odd, blk[r, q + 2, rows], blk[r, q, rows])
        red[q + 1, rows] = (total + sred[q + 1, rows]) * SIXTH

    def complete(r, q, t):
        row = TOP + 8 * t
        rows = pl.ds(row, 8)
        more = None
        if t == 0:
            more = jnp.where(sub == 0, blk[r, q + 1, pl.ds(row - 1, 8)], 0.0)
        if t == TILES - 1:
            more = jnp.where(sub == 7, blk[r, q + 1, pl.ds(row + 1, 8)], 0.0)
        side = None
        if q == 0:
            side = jnp.where(odd, 0.0, blk[r, 0, rows])
        if q == NQ - 1:
            side = jnp.where(odd, blk[r, 9, rows], 0.0)
        if side is not None:
            more = side if more is None else more + side
        if more is not None:
            red[q + 1, rows] = red[q + 1, rows] + more * SIXTH

    def halo_tiles(r, tiles):
        for t in tiles:
            row = TOP + 8 * t
            rows = pl.ds(row, 8)
            low, high = blk[r, 0, rows], blk[r, 9, rows]
            c, far = jnp.where(odd, high, low), jnp.where(odd, low, high)
            total = jnp.where(odd, blk[r, 0, pl.ds(row - 1, 8)], blk[r, 9, pl.ds(row - 1, 8)])
            total = total + jnp.where(odd, blk[r, 0, pl.ds(row + 1, 8)], blk[r, 9, pl.ds(row + 1, 8)])
            total = total + beside(c, xins[pl.ds(8 * (t // 8), 8)], slot(t, 0))
            total = total + far + jnp.where(odd, blk[r, 1, rows], blk[r, 8, rows])
            red[0, rows] = (total + sx[pl.ds(8 * t, 8)]) * inside

    def black_tile(r, q, t, final):
        rows = pl.ds(TOP + 8 * t, 8)
        total = around(red, (q + 1,), TOP + 8 * t, rins[pl.ds(8 * (t // 8), 8)], slot(t, q))
        above = (0 if q == NQ - 1 else q + 2) if isinstance(q, int) else q + 2
        total = total + jnp.where(odd, red[q, rows], red[above, rows])
        mine = pl.ds(8 * t, 8)
        value = (total + sblk[q, mine]) * SIXTH
        if final:
            other = red[q + 1, rows]
            merged[2 * q, mine] = jnp.where(odd, value, other)
            merged[2 * q + 1, mine] = jnp.where(odd, other, value)
        else:
            blk[r + 1, q + 1, rows] = value

    def finish_ends(r, final):
        for q in range(NQ):
            for t in (-1, TILES):
                red_beyond(r, q, t)
            for t in (0, 1, TILES - 2, TILES - 1):
                complete(r, q, t)
        halo_tiles(r, (0, 1, TILES - 2, TILES - 1))
        for q in range(NQ):
            for t in ENDS:
                black_tile(r, q, t, final)

    def finish_sides(r, final):
        for q in (0, NQ - 1):
            for t in range(2, TILES - 2):
                complete(r, q, t)
        halo_tiles(r, range(2, TILES - 2))
        for q in (0, NQ - 1):
            for t in range(1, TILES - 1):
                black_tile(r, q, t, final)

    return types.SimpleNamespace(**locals())


def kernel(
    field, source,
    blk, red, sred, sblk, ql, qr, qlo, qhi, sql, sqr, sx, merged,
    fld, src, elo, ehi, sqlo, sqhi, ins, xins, rins, sxs, sxd,
    load_sem, send_sem, recv_sem, ssend_sem, srecv_sem,
):
    def load(array, buffer, half, n):
        planes = pl.ds(4 * n, 4)
        return pltpu.make_async_copy(array.at[planes], buffer.at[planes], load_sem.at[half, n])

    for n in range(4):
        load(field, fld, 0, n).start()

    gx, gy, gz = (lax.axis_index(a) for a in ("gx", "gy", "gz"))
    nx, ny, nz = (lax.axis_size(a) for a in ("gx", "gy", "gz"))
    low_wall, high_wall = gx == 0, gx == nx - 1

    def device(d):
        return {
            "gx": gx + d[0],
            "gy": lax.rem(gy + d[1] + ny, ny),
            "gz": lax.rem(gz + d[2] + nz, nz),
        }

    def exists(d):
        if d[0] > 0:
            return gx < nx - 1
        if d[0] < 0:
            return gx > 0
        return None

    def opposite(d):
        return tuple(-v for v in d)

    def block_slices(d):
        dx, dy, _ = d
        sp, dp = ((8, 0) if dx > 0 else (1, 9)) if dx else (pl.ds(1, NQ), pl.ds(1, NQ))
        sr, dr = ((TOP + NY - 8, TOP - 8) if dy > 0 else (TOP, TOP + NY)) if dy else (TOP, TOP)
        n = 8 if dy else NY
        return (sp, pl.ds(sr, n)), (dp, pl.ds(dr, n))

    def refs(r, d):
        dx, dy, dz = d
        if dz == 0:
            s, t = block_slices(d)
            return blk.at[(r, *s)], blk.at[(r, *t)]
        col, dst = (qhi, ql) if dz > 0 else (qlo, qr)
        own = pl.ds(8, COLS)
        if dx:
            return col.at[r], dst.at[r, 0 if dx > 0 else 2, own]
        if dy:
            end, dr = (1, 0) if dy > 0 else (0, COLS + 8)
            return (ehi if dz > 0 else elo).at[r, end], dst.at[r, 1, pl.ds(dr, 8)]
        return col.at[r], dst.at[r, 1, own]

    def side(d):
        return 1 if d[0] > 0 else 2 if d[0] < 0 else 0

    def message(r, m):
        d = MESSAGES[m]
        s, t = refs(r, d)
        group = 3 if d in Z_FACES else side(d)
        return pltpu.make_async_remote_copy(
            src_ref=s, dst_ref=t, send_sem=send_sem.at[side(d)], recv_sem=recv_sem.at[r, group],
            device_id=device(d), device_id_type=MESH,
        )

    def smessage(m):
        d = FACES[m]
        if d[2]:
            s, t = (sqhi, sql) if d[2] > 0 else (sqlo, sqr)
        elif d[0]:
            n = side(d) - 1
            s, t = sxs.at[n], sxd.at[n]
        else:
            s, t = block_slices(d)
            s, t = sred.at[s], sred.at[t]
        group = 3 if d in Z_FACES else side(d)
        return pltpu.make_async_remote_copy(
            src_ref=s, dst_ref=t, send_sem=ssend_sem.at[side(d)], recv_sem=srecv_sem.at[group],
            device_id=device(d), device_id_type=MESH,
        )

    def start(make, dirs, select):
        for m, d in enumerate(dirs):
            if d in select:
                when(exists(d), lambda m=m: make(m).start())

    def wait(sem, kib):
        some = fld.at[pl.ds(0, 2), pl.ds(0, kib)]
        pltpu.make_async_copy(some, some, sem).wait()

    SIDE_KIB = 128 + 2 * 4 + 2 * 16

    def wait_sides(sems, kib, sent):
        when(exists((1 if sent else -1, 0, 0)), lambda: wait(sems(1), kib))
        when(exists((-1 if sent else 1, 0, 0)), lambda: wait(sems(2), kib))

    def arrived_z(r):
        wait(recv_sem.at[r, 3], 2 * 16)

    def arrived_rest(r):
        wait(recv_sem.at[r, 0], 4 * 4 + 2 * 32)
        wait_sides(lambda g: recv_sem.at[r, g], SIDE_KIB, False)

    def sent():
        wait(send_sem.at[0], 4 * 4 + 2 * 16 + 2 * 32)
        wait_sides(lambda g: send_sem.at[g], SIDE_KIB, True)

    def ssent():
        wait(ssend_sem.at[0], 2 * 16 + 2 * 32)
        wait_sides(lambda g: ssend_sem.at[g], 64, True)

    barrier = pltpu.get_barrier_semaphore()
    for d in MESSAGES:
        when(exists(d), lambda d=d: pl.semaphore_signal(barrier, inc=1, device_id=device(d), device_id_type=MESH))

    w = cells(blk, red, sred, sblk, ql, qr, qlo, qhi, sql, sqr, sx, merged, ins, xins, rins)
    sub, odd, half, half_after = w.sub, w.odd, w.half, w.half_after
    roll, slot, swap = w.roll, w.slot, w.swap

    def collect(lo, hi, lead, t, q, value, rows=None):
        m = slot(t, q)
        turned = roll(value, jnp.bitwise_and(2 * m + 2, NZ - 1))
        rows = pl.ds(8 * (t // 8), 8) if rows is None else rows
        hi[(*lead, rows)] = jnp.where(half == m, turned, hi[(*lead, rows)])
        lo[(*lead, rows)] = jnp.where(half_after == m, turned, lo[(*lead, rows)])

    def collect_edges(r):
        for end, t in enumerate(ENDS):
            for q in range(NQ):
                collect(elo, ehi, (r, end), t, q, blk[r, q + 1, pl.ds(TOP + 8 * t, 8)], pl.ds(0, 8))
            elo[r, end] = roll(elo[r, end], NZ - 2)

    def settle(lo, lead):
        for v in range(VECS):
            rows = pl.ds(8 * v, 8)
            lo[(*lead, rows)] = roll(lo[(*lead, rows)], NZ - 2)

    zero = jnp.zeros((ROWS, NZ), jnp.float32)

    def wall(pair, plane):
        for r in range(SWEEPS):
            blk[r, pair] = zero
            ql[r, plane] = jnp.zeros((COLS + 16, NZ), jnp.float32)
            qr[r, plane] = jnp.zeros((COLS + 16, NZ), jnp.float32)
        sxd[0 if pair == 0 else 1] = jnp.zeros((NY // 2, NZ), jnp.float32)

    pl.when(low_wall)(lambda: wall(0, 0))
    pl.when(high_wall)(lambda: wall(9, 2))
    def pack_field(q, c):
        for t in range(TILES):
            rows = pl.ds(8 * t, 8)
            value = jnp.where(odd, fld[2 * q, rows], fld[2 * q + 1, rows])
            blk[0, q + 1, pl.ds(TOP + 8 * t, 8)] = value
            collect(qlo, qhi, (0,), t, q, value)
        return c

    def packed_field(n, c):
        load(field, fld, 0, n).wait()
        load(source, src, 1, n).start()
        return pack_field(2 * n + 1, pack_field(2 * n, c))

    lax.fori_loop(0, 4, packed_field, 0)
    collect_edges(0)
    settle(qlo, (0,))

    walls = jnp.where(jnp.logical_or(low_wall, high_wall), 1, 0)
    pl.semaphore_wait(barrier, len(MESSAGES) - 5 * walls)
    start(functools.partial(message, 0), MESSAGES, MESSAGES)

    def pack_source(q, c):
        for t in range(TILES):
            rows = pl.ds(8 * t, 8)
            even_plane, odd_plane = src[2 * q, rows], src[2 * q + 1, rows]
            value = jnp.where(odd, odd_plane, even_plane)
            sred[q + 1, pl.ds(TOP + 8 * t, 8)] = value
            sblk[q, rows] = jnp.where(odd, even_plane, odd_plane)
            collect(sqlo, sqhi, (), t, q, value)
        return c

    def packed_source(n, c):
        load(source, src, 1, n).wait()
        return pack_source(2 * n + 1, pack_source(2 * n, c))

    lax.fori_loop(0, 4, packed_source, 0)
    settle(sqlo, ())
    start(smessage, FACES, Z_FACES + Y_FACES)
    for t in range(TILES // 2):
        near, away = pl.ds(TOP + 8 * t, 8), pl.ds(TOP + 8 * t + NY // 2, 8)
        sxs[0, pl.ds(8 * t, 8)] = jnp.where(odd, sred[NQ, near], swap(sred[NQ, away]))
        sxs[1, pl.ds(8 * t, 8)] = jnp.where(odd, swap(sred[1, away]), sred[1, near])
    start(smessage, FACES, X_FACES)

    def sweep(r, final):
        for q in range(NQ):
            for t in range(TILES):
                w.red_tile(r, q, t)
        arrived_z(r)
        pl.when(r == 0)(lambda: wait(srecv_sem.at[3], 2 * 16))

        w.columns(r, False)

        for q in range(NQ):
            for t in range(TILES):
                w.complete_z(q, t)

        def black_inner(n, c):
            for q in (3 * n + 1, 3 * n + 2, 3 * n + 3):
                for t in range(1, TILES - 1):
                    w.black_tile(r, q, t, final)
            return c

        lax.fori_loop(0, 2, black_inner, 0)
        if not final:
            for t in range(1, TILES - 1):
                for q in range(1, NQ - 1):
                    collect(qlo, qhi, (r + 1,), t, q, blk[r + 1, q + 1, pl.ds(TOP + 8 * t, 8)])

        arrived_rest(r)

        @pl.when(r == 0)
        def _():
            wait(srecv_sem.at[0], 2 * 32)
            wait_sides(lambda g: srecv_sem.at[g], 64, False)
            for t in range(TILES // 2):
                low, high = sxd[0, pl.ds(8 * t, 8)], sxd[1, pl.ds(8 * t, 8)]
                sx[pl.ds(8 * t, 8)] = jnp.where(odd, low, high)
                sx[pl.ds(8 * t + NY // 2, 8)] = swap(jnp.where(odd, high, low))

        sent()
        if final:
            return
        w.columns(r, True)
        w.finish_ends(r, False)
        after = functools.partial(message, r + 1)
        collect_edges(r + 1)
        start(after, MESSAGES, YZ_EDGES + XY_EDGES + Y_FACES)
        w.finish_sides(r, False)
        for t in range(TILES):
            for q in range(NQ) if t in ENDS else (0, NQ - 1):
                collect(qlo, qhi, (r + 1,), t, q, blk[r + 1, q + 1, pl.ds(TOP + 8 * t, 8)])
        settle(qlo, (r + 1,))
        start(after, MESSAGES, XZ_EDGES + Z_FACES + X_FACES)

    def sweeps(r, c):
        sweep(r, False)
        return c

    lax.fori_loop(0, SWEEPS - 1, sweeps, 0)
    sweep(SWEEPS - 1, True)
    ssent()


def finish(
    blk, red_in, sred, sblk, ql, qr, qlo, qhi, sql, sqr, sx, merged, out, red,
    late, ins, xins, rins, sem,
):
    del red_in
    w = cells(blk, red, sred, sblk, ql, qr, qlo, qhi, sql, sqr, sx, late, ins, xins, rins)

    def store(n):
        planes, rows = [
            (pl.ds(2, 2 * NQ - 4), pl.ds(8, NY - 16)),
            (pl.ds(2, 2 * NQ - 4), pl.ds(0, 8)),
            (pl.ds(2, 2 * NQ - 4), pl.ds(NY - 8, 8)),
            (pl.ds(0, 2), pl.ds(0, NY)),
            (pl.ds(2 * NQ - 2, 2), pl.ds(0, NY)),
        ][n]
        origin = merged if n == 0 else late
        return pltpu.make_async_copy(origin.at[planes, rows], out.at[planes, rows], sem.at[n])

    store(0).start()
    r = SWEEPS - 1
    w.columns(r, True)
    w.finish_ends(r, True)
    store(1).start()
    store(2).start()
    w.finish_sides(r, True)
    store(3).start()
    store(4).start()
    for n in range(5):
        store(n).wait()


def on_device(field, source):
    f32 = jnp.float32
    dma = pltpu.SemaphoreType.DMA
    columns = (COLS, NZ)
    shared = [
        (SWEEPS, NQ + 2, ROWS, NZ),
        (NQ + 1, ROWS, NZ),
        (NQ + 2, ROWS, NZ),
        (NQ, NY, NZ),
        (SWEEPS, 3, COLS + 16, NZ),
        (SWEEPS, 3, COLS + 16, NZ),
        (SWEEPS, *columns),
        (SWEEPS, *columns),
        columns,
        columns,
        (NY, NZ),
        (2 * NQ, NY, NZ),
    ]
    vmem, hbm = (pl.BlockSpec(memory_space=m) for m in (pltpu.VMEM, pltpu.HBM))
    inserts = [pltpu.VMEM(shape, f32) for shape in ((COLS + 16, NZ), columns, columns)]
    field, source = (pltpu.with_memory_space_constraint(x, pltpu.HBM) for x in (field, source))
    state = pl.pallas_call(
        kernel,
        name="smooth",
        out_shape=[pltpu.VMEM(shape, f32) for shape in shared],
        in_specs=[hbm] * 2,
        out_specs=[vmem] * len(shared),
        scratch_shapes=[
            pltpu.VMEM((2 * NQ, NY, NZ), f32),
            pltpu.VMEM((2 * NQ, NY, NZ), f32),
            pltpu.VMEM((SWEEPS, 2, 8, NZ), f32),
            pltpu.VMEM((SWEEPS, 2, 8, NZ), f32),
            pltpu.VMEM(columns, f32),
            pltpu.VMEM(columns, f32),
            *inserts,
            pltpu.VMEM((2, NY // 2, NZ), f32),
            pltpu.VMEM((2, NY // 2, NZ), f32),
            dma((2, 4)),
            dma((3,)),
            dma((SWEEPS, 4)),
            dma((3,)),
            dma((4,)),
        ],
        compiler_params=pltpu.CompilerParams(
            collective_id=0, has_side_effects=True, vmem_limit_bytes=VMEM_GRANT
        ),
    )(field, source)
    state = [pltpu.with_memory_space_constraint(x, pltpu.VMEM) for x in state]
    result, _ = pl.pallas_call(
        finish,
        name="finish",
        out_shape=[jax.ShapeDtypeStruct(field.shape, f32), pltpu.VMEM(shared[1], f32)],
        in_specs=[vmem] * len(shared),
        out_specs=[hbm, vmem],
        input_output_aliases={1: 1},
        scratch_shapes=[pltpu.VMEM((2 * NQ, NY, NZ), f32), *inserts, dma((5,))],
        compiler_params=pltpu.CompilerParams(vmem_limit_bytes=VMEM_GRANT),
    )(*state)
    return result


def solution(mesh):
    spec = P("gx", "gy", "gz")
    return jax.shard_map(
        on_device, mesh=mesh, in_specs=(spec, spec), out_specs=spec, check_vma=False
    )
```

```python
import functools
import itertools
import types

import jax
import jax.numpy as jnp
from jax import lax
from jax.experimental import pallas as pl
from jax.experimental.pallas import tpu as pltpu
from jax.sharding import PartitionSpec as P

MESH = pl.DeviceIdType.MESH
SWEEPS = 3
NQ, NY, NZ = 8, 256, 128
TILES = NY // 8
ENDS = (0, TILES - 1)
TOP = 16
ROWS = NY + 2 * TOP
VECS = TILES // 8
COLS = 8 * VECS
SIXTH = 1.0 / 6.0
VMEM_GRANT = 24 << 20
FIRST_ROWS = 192

EDGES = [d for d in itertools.product((-1, 0, 1), repeat=3) if sum(map(abs, d)) == 2]
FACES = [(0, 0, 1), (0, 0, -1), (0, 1, 0), (0, -1, 0), (1, 0, 0), (-1, 0, 0)]
MESSAGES = [d for d in EDGES if d[0] == 0] + [d for d in EDGES if d[0]] + FACES
X_FACES, Y_FACES, Z_FACES = FACES[4:], FACES[2:4], FACES[:2]
YZ_EDGES, XY_EDGES, XZ_EDGES = ([d for d in EDGES if d[a] == 0] for a in (0, 2, 1))


def when(cond, f):
    if cond is None:
        f()
    else:
        pl.when(cond)(f)


def cells(blk, red, sred, sblk, ql, qr, xq, qlo, qhi, sql, sqr, sx, merged, ins, xins, rins):
    gx = lax.axis_index("gx")
    low_wall, high_wall = gx == 0, gx == lax.axis_size("gx") - 1
    lane = lax.broadcasted_iota(jnp.int32, (8, NZ), 1)
    sub = lax.broadcasted_iota(jnp.int32, (8, NZ), 0)
    odd = jnp.bitwise_and(lane + sub, 1) == 1
    even_lane = jnp.bitwise_and(lane, 1) == 0
    first, last = lane == 0, lane == NZ - 1
    outer = jnp.logical_or(first, last)
    group = jnp.bitwise_and(lane, 15)
    half = jnp.right_shift(lane, 1)
    half_after = jnp.bitwise_and(half - 1, NZ // 2 - 1)

    def roll(x, shift):
        return pltpu.roll(x, shift, 1)

    def slot(t, q):
        return 8 * (t % 8) + q

    inside = jnp.where(odd, jnp.where(low_wall, 0.0, SIXTH), jnp.where(high_wall, 0.0, SIXTH))

    def swap(x):
        return jnp.where(jnp.bitwise_and(sub, 1) == 0, pltpu.roll(x, 7, 0), pltpu.roll(x, 1, 0))

    def columns(r, edges):
        for v in range(-1, VECS + 1) if edges else range(VECS):
            rows = pl.ds(8 * v + 8, 8)
            ins[rows] = jnp.where(even_lane, qr[r, rows], ql[r, rows])
        for v in range(VECS):
            here, rows = pl.ds(8 * v + 8, 8), pl.ds(8 * v, 8)
            c = ins[here]
            before = ins[rows] if edges or v > 0 else c
            after = ins[pl.ds(8 * v + 16, 8)] if edges or v < VECS - 1 else c
            back = roll(jnp.where(lane >= NZ - 16, before, c), 16)
            ahead = roll(jnp.where(lane < 16, after, c), NZ - 16)
            total = c + jnp.where(sub == 0, pltpu.roll(back, 1, 0), pltpu.roll(c, 1, 0))
            total = total + jnp.where(sub == 7, pltpu.roll(ahead, 7, 0), pltpu.roll(c, 7, 0))
            up, down = roll(c, NZ - 2), roll(c, 2)
            if edges:
                above = jnp.where(even_lane, xq[r, 1, 1], xq[r, 1, 0])
                below = jnp.where(even_lane, xq[r, 0, 1], xq[r, 0, 0])
                back = (NZ - 2 * v) % NZ
                below = roll(below, back)
                up = jnp.where(group >= 14, roll(above, 14 - 2 * v), up)
                down = jnp.where(group < 2, below, down)
                xins[rows] = jnp.where(odd, roll(above, back), below)
            total = total + jnp.where(odd, up, down)
            left, right = ql[r, here] + qlo[r, rows], qr[r, here] + qhi[r, rows]
            total = total + jnp.where(even_lane, roll(right, NZ - 1), roll(left, 1))
            total = total + jnp.where(even_lane, sqr[rows], sql[rows])
            rins[rows] = total * SIXTH

    def beside(c, edge, m):
        edge = roll(edge, NZ - 1 - 2 * m)
        return jnp.where(first, edge, roll(c, 1)) + jnp.where(last, edge, roll(c, NZ - 1))

    def around(ref, lead, row, edge, m):
        c = ref[(*lead, pl.ds(row, 8))]
        total = c + ref[(*lead, pl.ds(row - 1, 8))] + ref[(*lead, pl.ds(row + 1, 8))]
        return total + beside(c, edge, m)

    def red_tile(r, q, t):
        row = TOP + 8 * t
        rows = pl.ds(row, 8)
        c = blk[r, q + 1, rows]
        total = c + jnp.where(first, 0.0, roll(c, 1)) + jnp.where(last, 0.0, roll(c, NZ - 1))
        up = jnp.where(sub == 0, 0.0, pltpu.roll(c, 1, 0)) if t == 0 else blk[r, q + 1, pl.ds(row - 1, 8)]
        down = jnp.where(sub == 7, 0.0, pltpu.roll(c, 7, 0)) if t == TILES - 1 else blk[r, q + 1, pl.ds(row + 1, 8)]
        above = blk[r, q + 2, rows] if q < NQ - 1 else 0.0
        below = blk[r, q, rows] if q > 0 else 0.0
        total = total + up + down + jnp.where(odd, above, below)
        red[q + 1, rows] = (total + sred[q + 1, rows]) * SIXTH

    def complete_z(q, t):
        rows = pl.ds(TOP + 8 * t, 8)
        edge = roll(ins[pl.ds(8 * (t // 8) + 8, 8)], NZ - 1 - 2 * slot(t, q))
        red[q + 1, rows] = red[q + 1, rows] + jnp.where(outer, edge, 0.0) * SIXTH

    def red_beyond(r, q, t):
        rows = pl.ds(TOP + 8 * t, 8)
        total = around(blk, (r, q + 1), TOP + 8 * t, ins[pl.ds(8 * (t // 8) + 8, 8)], slot(t, q))
        total = total + jnp.where(odd, blk[r, q + 2, rows], blk[r, q, rows])
        red[q + 1, rows] = (total + sred[q + 1, rows]) * SIXTH

    def complete(r, q, t):
        row = TOP + 8 * t
        rows = pl.ds(row, 8)
        more = None
        if t == 0:
            more = jnp.where(sub == 0, blk[r, q + 1, pl.ds(row - 1, 8)], 0.0)
        if t == TILES - 1:
            more = jnp.where(sub == 7, blk[r, q + 1, pl.ds(row + 1, 8)], 0.0)
        side = None
        if q == 0:
            side = jnp.where(odd, 0.0, blk[r, 0, rows])
        if q == NQ - 1:
            side = jnp.where(odd, blk[r, 9, rows], 0.0)
        if side is not None:
            more = side if more is None else more + side
        if more is not None:
            red[q + 1, rows] = red[q + 1, rows] + more * SIXTH

    def halo_tiles(r, tiles):
        for t in tiles:
            row = TOP + 8 * t
            rows = pl.ds(row, 8)
            low, high = blk[r, 0, rows], blk[r, 9, rows]
            c, far = jnp.where(odd, high, low), jnp.where(odd, low, high)
            total = jnp.where(odd, blk[r, 0, pl.ds(row - 1, 8)], blk[r, 9, pl.ds(row - 1, 8)])
            total = total + jnp.where(odd, blk[r, 0, pl.ds(row + 1, 8)], blk[r, 9, pl.ds(row + 1, 8)])
            total = total + beside(c, xins[pl.ds(8 * (t // 8), 8)], slot(t, 0))
            total = total + far + jnp.where(odd, blk[r, 1, rows], blk[r, 8, rows])
            red[0, rows] = (total + sx[pl.ds(8 * t, 8)]) * inside

    def black_tile(r, q, t, final):
        rows = pl.ds(TOP + 8 * t, 8)
        total = around(red, (q + 1,), TOP + 8 * t, rins[pl.ds(8 * (t // 8), 8)], slot(t, q))
        above = (0 if q == NQ - 1 else q + 2) if isinstance(q, int) else q + 2
        total = total + jnp.where(odd, red[q, rows], red[above, rows])
        mine = pl.ds(8 * t, 8)
        value = (total + sblk[q, mine]) * SIXTH
        if final:
            other = red[q + 1, rows]
            merged[2 * q, mine] = jnp.where(odd, value, other)
            merged[2 * q + 1, mine] = jnp.where(odd, other, value)
        else:
            blk[r + 1, q + 1, rows] = value

    def finish_ends(r, final):
        for q in range(NQ):
            for t in (-1, TILES):
                red_beyond(r, q, t)
            for t in (0, 1, TILES - 2, TILES - 1):
                complete(r, q, t)
        halo_tiles(r, (0, 1, TILES - 2, TILES - 1))
        for q in range(NQ):
            for t in ENDS:
                black_tile(r, q, t, final)

    def finish_sides(r, final):
        for q in (0, NQ - 1):
            for t in range(2, TILES - 2):
                complete(r, q, t)
        halo_tiles(r, range(2, TILES - 2))
        for q in (0, NQ - 1):
            for t in range(1, TILES - 1):
                black_tile(r, q, t, final)

    return types.SimpleNamespace(**locals())


def kernel(
    field, source,
    blk, red, sred, sblk, ql, qr, xq, qlo, qhi, sql, sqr, sx, merged,
    fld, src, elo, ehi, xe, sqlo, sqhi, ins, xins, rins, sxs, sxd,
    load_sem, send_sem, recv_sem, ssend_sem, srecv_sem,
):
    def load(array, buffer, half, n):
        planes = pl.ds(4 * n, 4)
        return pltpu.make_async_copy(array.at[planes], buffer.at[planes], load_sem.at[half, n])

    for n in range(4):
        load(field, fld, 0, n).start()

    gx, gy, gz = (lax.axis_index(a) for a in ("gx", "gy", "gz"))
    nx, ny, nz = (lax.axis_size(a) for a in ("gx", "gy", "gz"))
    low_wall, high_wall = gx == 0, gx == nx - 1

    def device(d):
        return {
            "gx": gx + d[0],
            "gy": lax.rem(gy + d[1] + ny, ny),
            "gz": lax.rem(gz + d[2] + nz, nz),
        }

    def exists(d):
        if d[0] > 0:
            return gx < nx - 1
        if d[0] < 0:
            return gx > 0
        return None

    def opposite(d):
        return tuple(-v for v in d)

    def block_slices(d):
        dx, dy, _ = d
        sp, dp = ((8, 0) if dx > 0 else (1, 9)) if dx else (pl.ds(1, NQ), pl.ds(1, NQ))
        sr, dr = ((TOP + NY - 8, TOP - 8) if dy > 0 else (TOP, TOP + NY)) if dy else (TOP, TOP)
        n = 8 if dy else NY
        return (sp, pl.ds(sr, n)), (dp, pl.ds(dr, n))

    def refs(r, d):
        dx, dy, dz = d
        if dz == 0:
            s, t = block_slices(d)
            return blk.at[(r, *s)], blk.at[(r, *t)]
        col, dst = (qhi, ql) if dz > 0 else (qlo, qr)
        own = pl.ds(8, COLS)
        if dx:
            place = (r, 0 if dx > 0 else 1, 0 if dz > 0 else 1)
            return xe.at[place], xq.at[place]
        if dy:
            end, dr = (1, 0) if dy > 0 else (0, COLS + 8)
            return (ehi if dz > 0 else elo).at[r, end], dst.at[r, pl.ds(dr, 8)]
        return col.at[r], dst.at[r, own]

    def side(d):
        return 1 if d[0] > 0 else 2 if d[0] < 0 else 0

    def message(r, m):
        d = MESSAGES[m]
        s, t = refs(r, d)
        group = 3 if d in Z_FACES else side(d)
        return pltpu.make_async_remote_copy(
            src_ref=s, dst_ref=t, send_sem=send_sem.at[side(d)], recv_sem=recv_sem.at[r, group],
            device_id=device(d), device_id_type=MESH,
        )

    def smessage(m):
        d = FACES[m]
        if d[2]:
            s, t = (sqhi, sql) if d[2] > 0 else (sqlo, sqr)
        elif d[0]:
            n = side(d) - 1
            s, t = sxs.at[n], sxd.at[n]
        else:
            s, t = block_slices(d)
            s, t = sred.at[s], sred.at[t]
        group = 3 if d in Z_FACES else side(d)
        return pltpu.make_async_remote_copy(
            src_ref=s, dst_ref=t, send_sem=ssend_sem.at[side(d)], recv_sem=srecv_sem.at[group],
            device_id=device(d), device_id_type=MESH,
        )

    def start(make, dirs, select):
        for m, d in enumerate(dirs):
            if d in select:
                when(exists(d), lambda m=m: make(m).start())

    def wait(sem, kib):
        some = fld.at[pl.ds(0, 2), pl.ds(0, kib)]
        pltpu.make_async_copy(some, some, sem).wait()

    SIDE_KIB = 128 + 4 * 4

    def wait_sides(sems, kib, sent):
        when(exists((1 if sent else -1, 0, 0)), lambda: wait(sems(1), kib))
        when(exists((-1 if sent else 1, 0, 0)), lambda: wait(sems(2), kib))

    def arrived_z(r):
        wait(recv_sem.at[r, 3], 2 * 16)

    def arrived_rest(r):
        wait(recv_sem.at[r, 0], 4 * 4 + 2 * 32)
        wait_sides(lambda g: recv_sem.at[r, g], SIDE_KIB, False)

    def sent():
        wait(send_sem.at[0], 4 * 4 + 2 * 16 + 2 * 32)
        wait_sides(lambda g: send_sem.at[g], SIDE_KIB, True)

    def ssent():
        wait(ssend_sem.at[0], 2 * 16 + 2 * 32)
        wait_sides(lambda g: ssend_sem.at[g], 64, True)

    barrier = pltpu.get_barrier_semaphore()
    for d in MESSAGES:
        when(exists(d), lambda d=d: pl.semaphore_signal(barrier, inc=1, device_id=device(d), device_id_type=MESH))

    w = cells(blk, red, sred, sblk, ql, qr, xq, qlo, qhi, sql, sqr, sx, merged, ins, xins, rins)
    sub, odd, half, half_after = w.sub, w.odd, w.half, w.half_after
    roll, slot, swap = w.roll, w.slot, w.swap

    def collect(lo, hi, lead, t, q, value, rows=None):
        m = slot(t, q)
        turned = roll(value, jnp.bitwise_and(2 * m + 2, NZ - 1))
        rows = pl.ds(8 * (t // 8), 8) if rows is None else rows
        hi[(*lead, rows)] = jnp.where(half == m, turned, hi[(*lead, rows)])
        lo[(*lead, rows)] = jnp.where(half_after == m, turned, lo[(*lead, rows)])

    def collect_edges(r):
        for end, t in enumerate(ENDS):
            for q in range(NQ):
                collect(elo, ehi, (r, end), t, q, blk[r, q + 1, pl.ds(TOP + 8 * t, 8)], pl.ds(0, 8))
            elo[r, end] = roll(elo[r, end], NZ - 2)

    def settle(lo, lead):
        for v in range(VECS):
            rows = pl.ds(8 * v, 8)
            lo[(*lead, rows)] = roll(lo[(*lead, rows)], NZ - 2)

    def collect_xz(r):
        for place, pair in enumerate((NQ - 1, 0)):
            for z, col in enumerate((qhi, qlo)):
                piece = roll(col[r, pl.ds(0, 8)], (NZ - 2 * pair) % NZ)
                for v in range(1, VECS):
                    more = roll(col[r, pl.ds(8 * v, 8)], (2 * v - 2 * pair) % NZ)
                    piece = jnp.where(jnp.right_shift(w.group, 1) == v, more, piece)
                xe[r, place, z] = piece

    zero = jnp.zeros((ROWS, NZ), jnp.float32)

    def wall(pair, plane):
        for r in range(SWEEPS):
            blk[r, pair] = zero
            for z in range(2):
                xq[r, plane, z] = jnp.zeros((8, NZ), jnp.float32)
        sxd[0 if pair == 0 else 1] = jnp.zeros((NY // 2, NZ), jnp.float32)

    pl.when(low_wall)(lambda: wall(0, 0))
    pl.when(high_wall)(lambda: wall(9, 1))
    def pack_field(q, c):
        for t in range(TILES):
            rows = pl.ds(8 * t, 8)
            value = jnp.where(odd, fld[2 * q, rows], fld[2 * q + 1, rows])
            blk[0, q + 1, pl.ds(TOP + 8 * t, 8)] = value
            collect(qlo, qhi, (0,), t, q, value)
        return c

    def packed_field(n, c):
        load(field, fld, 0, n).wait()
        load(source, src, 1, n).start()
        return pack_field(2 * n + 1, pack_field(2 * n, c))

    lax.fori_loop(0, 4, packed_field, 0)
    collect_edges(0)
    settle(qlo, (0,))
    collect_xz(0)

    walls = jnp.where(jnp.logical_or(low_wall, high_wall), 1, 0)
    pl.semaphore_wait(barrier, len(MESSAGES) - 5 * walls)
    start(functools.partial(message, 0), MESSAGES, EDGES + Z_FACES + Y_FACES)

    def x_face(m, row, n):
        d = FACES[m]
        sp, dp = (8, 0) if d[0] > 0 else (1, 9)
        rows = pl.ds(TOP + row, n)
        return pltpu.make_async_remote_copy(
            src_ref=blk.at[0, sp, rows], dst_ref=blk.at[0, dp, rows],
            send_sem=send_sem.at[side(d)], recv_sem=recv_sem.at[0, side(d)],
            device_id=device(d), device_id_type=MESH,
        )

    start(lambda m: x_face(m, 0, FIRST_ROWS), FACES, X_FACES)

    def pack_source(q, c):
        for t in range(TILES):
            rows = pl.ds(8 * t, 8)
            even_plane, odd_plane = src[2 * q, rows], src[2 * q + 1, rows]
            value = jnp.where(odd, odd_plane, even_plane)
            sred[q + 1, pl.ds(TOP + 8 * t, 8)] = value
            sblk[q, rows] = jnp.where(odd, even_plane, odd_plane)
            collect(sqlo, sqhi, (), t, q, value)
        return c

    def packed_source(n, c):
        load(source, src, 1, n).wait()
        return pack_source(2 * n + 1, pack_source(2 * n, c))

    lax.fori_loop(0, 4, packed_source, 0)
    settle(sqlo, ())
    start(smessage, FACES, Z_FACES + Y_FACES)
    start(lambda m: x_face(m, FIRST_ROWS, NY - FIRST_ROWS), FACES, X_FACES)
    for t in range(TILES // 2):
        near, away = pl.ds(TOP + 8 * t, 8), pl.ds(TOP + 8 * t + NY // 2, 8)
        sxs[0, pl.ds(8 * t, 8)] = jnp.where(odd, sred[NQ, near], swap(sred[NQ, away]))
        sxs[1, pl.ds(8 * t, 8)] = jnp.where(odd, swap(sred[1, away]), sred[1, near])
    start(smessage, FACES, X_FACES)

    def sweep(r, final):
        for q in range(NQ):
            for t in range(TILES):
                w.red_tile(r, q, t)
        arrived_z(r)
        pl.when(r == 0)(lambda: wait(srecv_sem.at[3], 2 * 16))

        w.columns(r, False)

        for q in range(NQ):
            for t in range(TILES):
                w.complete_z(q, t)

        def black_inner(n, c):
            for q in (3 * n + 1, 3 * n + 2, 3 * n + 3):
                for t in range(1, TILES - 1):
                    w.black_tile(r, q, t, final)
            return c

        lax.fori_loop(0, 2, black_inner, 0)
        if not final:
            for t in range(1, TILES - 1):
                for q in range(1, NQ - 1):
                    collect(qlo, qhi, (r + 1,), t, q, blk[r + 1, q + 1, pl.ds(TOP + 8 * t, 8)])

        arrived_rest(r)

        @pl.when(r == 0)
        def _():
            wait(srecv_sem.at[0], 2 * 32)
            wait_sides(lambda g: srecv_sem.at[g], 64, False)
            for t in range(TILES // 2):
                low, high = sxd[0, pl.ds(8 * t, 8)], sxd[1, pl.ds(8 * t, 8)]
                sx[pl.ds(8 * t, 8)] = jnp.where(odd, low, high)
                sx[pl.ds(8 * t + NY // 2, 8)] = swap(jnp.where(odd, high, low))

        sent()
        if final:
            return
        w.columns(r, True)
        w.finish_ends(r, False)
        after = functools.partial(message, r + 1)
        collect_edges(r + 1)
        start(after, MESSAGES, YZ_EDGES + XY_EDGES + Y_FACES)
        w.finish_sides(r, False)
        for t in range(TILES):
            for q in range(NQ) if t in ENDS else (0, NQ - 1):
                collect(qlo, qhi, (r + 1,), t, q, blk[r + 1, q + 1, pl.ds(TOP + 8 * t, 8)])
        settle(qlo, (r + 1,))
        start(after, MESSAGES, Z_FACES)
        collect_xz(r + 1)
        start(after, MESSAGES, XZ_EDGES + X_FACES)

    def sweeps(r, c):
        sweep(r, False)
        return c

    lax.fori_loop(0, SWEEPS - 1, sweeps, 0)
    sweep(SWEEPS - 1, True)
    ssent()


def finish(
    blk, red_in, sred, sblk, ql, qr, xq, qlo, qhi, sql, sqr, sx, merged, out, red,
    late, ins, xins, rins, sem,
):
    del red_in
    w = cells(blk, red, sred, sblk, ql, qr, xq, qlo, qhi, sql, sqr, sx, late, ins, xins, rins)

    def store(n):
        planes, rows = [
            (pl.ds(2, 2 * NQ - 4), pl.ds(8, NY - 16)),
            (pl.ds(2, 2 * NQ - 4), pl.ds(0, 8)),
            (pl.ds(2, 2 * NQ - 4), pl.ds(NY - 8, 8)),
            (pl.ds(0, 2), pl.ds(0, NY)),
            (pl.ds(2 * NQ - 2, 2), pl.ds(0, NY)),
        ][n]
        origin = merged if n == 0 else late
        return pltpu.make_async_copy(origin.at[planes, rows], out.at[planes, rows], sem.at[n])

    store(0).start()
    r = SWEEPS - 1
    w.columns(r, True)
    w.finish_ends(r, True)
    store(1).start()
    store(2).start()
    w.finish_sides(r, True)
    store(3).start()
    store(4).start()
    for n in range(5):
        store(n).wait()


def on_device(field, source):
    f32 = jnp.float32
    dma = pltpu.SemaphoreType.DMA
    columns = (COLS, NZ)
    shared = [
        (SWEEPS, NQ + 2, ROWS, NZ),
        (NQ + 1, ROWS, NZ),
        (NQ + 2, ROWS, NZ),
        (NQ, NY, NZ),
        (SWEEPS, COLS + 16, NZ),
        (SWEEPS, COLS + 16, NZ),
        (SWEEPS, 2, 2, 8, NZ),
        (SWEEPS, *columns),
        (SWEEPS, *columns),
        columns,
        columns,
        (NY, NZ),
        (2 * NQ, NY, NZ),
    ]
    vmem, hbm = (pl.BlockSpec(memory_space=m) for m in (pltpu.VMEM, pltpu.HBM))
    inserts = [pltpu.VMEM(shape, f32) for shape in ((COLS + 16, NZ), columns, columns)]
    field, source = (pltpu.with_memory_space_constraint(x, pltpu.HBM) for x in (field, source))
    state = pl.pallas_call(
        kernel,
        name="smooth",
        out_shape=[pltpu.VMEM(shape, f32) for shape in shared],
        in_specs=[hbm] * 2,
        out_specs=[vmem] * len(shared),
        scratch_shapes=[
            pltpu.VMEM((2 * NQ, NY, NZ), f32),
            pltpu.VMEM((2 * NQ, NY, NZ), f32),
            pltpu.VMEM((SWEEPS, 2, 8, NZ), f32),
            pltpu.VMEM((SWEEPS, 2, 8, NZ), f32),
            pltpu.VMEM((SWEEPS, 2, 2, 8, NZ), f32),
            pltpu.VMEM(columns, f32),
            pltpu.VMEM(columns, f32),
            *inserts,
            pltpu.VMEM((2, NY // 2, NZ), f32),
            pltpu.VMEM((2, NY // 2, NZ), f32),
            dma((2, 4)),
            dma((3,)),
            dma((SWEEPS, 4)),
            dma((3,)),
            dma((4,)),
        ],
        compiler_params=pltpu.CompilerParams(
            collective_id=0, has_side_effects=True, vmem_limit_bytes=VMEM_GRANT
        ),
    )(field, source)
    state = [pltpu.with_memory_space_constraint(x, pltpu.VMEM) for x in state]
    result, _ = pl.pallas_call(
        finish,
        name="finish",
        out_shape=[jax.ShapeDtypeStruct(field.shape, f32), pltpu.VMEM(shared[1], f32)],
        in_specs=[vmem] * len(shared),
        out_specs=[hbm, vmem],
        input_output_aliases={1: 1},
        scratch_shapes=[pltpu.VMEM((2 * NQ, NY, NZ), f32), *inserts, dma((5,))],
        compiler_params=pltpu.CompilerParams(vmem_limit_bytes=VMEM_GRANT),
    )(*state)
    return result


def solution(mesh):
    spec = P("gx", "gy", "gz")
    return jax.shard_map(
        on_device, mesh=mesh, in_specs=(spec, spec), out_specs=spec, check_vma=False
    )
```

```python
import functools
import itertools
import types

import jax
import jax.numpy as jnp
from jax import lax
from jax.experimental import pallas as pl
from jax.experimental.pallas import tpu as pltpu
from jax.sharding import PartitionSpec as P

MESH = pl.DeviceIdType.MESH
SWEEPS = 3
NQ, NY, NZ = 8, 256, 128
TILES = NY // 8
ENDS = (0, TILES - 1)
TOP = 16
ROWS = NY + 2 * TOP
VECS = TILES // 8
COLS = 8 * VECS
SIXTH = 1.0 / 6.0
VMEM_GRANT = 24 << 20

EDGES = [d for d in itertools.product((-1, 0, 1), repeat=3) if sum(map(abs, d)) == 2]
FACES = [(0, 0, 1), (0, 0, -1), (0, 1, 0), (0, -1, 0), (1, 0, 0), (-1, 0, 0)]
MESSAGES = [d for d in EDGES if d[0] == 0] + [d for d in EDGES if d[0]] + FACES
X_FACES, Y_FACES, Z_FACES = FACES[4:], FACES[2:4], FACES[:2]
YZ_EDGES, XY_EDGES, XZ_EDGES = ([d for d in EDGES if d[a] == 0] for a in (0, 2, 1))


def when(cond, f):
    if cond is None:
        f()
    else:
        pl.when(cond)(f)


def cells(blk, red, sred, sblk, ql, qr, xq, qlo, qhi, sql, sqr, sx, merged, ins, xins, rins):
    gx = lax.axis_index("gx")
    low_wall, high_wall = gx == 0, gx == lax.axis_size("gx") - 1
    lane = lax.broadcasted_iota(jnp.int32, (8, NZ), 1)
    sub = lax.broadcasted_iota(jnp.int32, (8, NZ), 0)
    odd = jnp.bitwise_and(lane + sub, 1) == 1
    even_lane = jnp.bitwise_and(lane, 1) == 0
    first, last = lane == 0, lane == NZ - 1
    outer = jnp.logical_or(first, last)
    group = jnp.bitwise_and(lane, 15)
    half = jnp.right_shift(lane, 1)
    half_after = jnp.bitwise_and(half - 1, NZ // 2 - 1)

    def roll(x, shift):
        return pltpu.roll(x, shift, 1)

    def slot(t, q):
        return 8 * (t % 8) + q

    inside = jnp.where(odd, jnp.where(low_wall, 0.0, SIXTH), jnp.where(high_wall, 0.0, SIXTH))

    def swap(x):
        return jnp.where(jnp.bitwise_and(sub, 1) == 0, pltpu.roll(x, 7, 0), pltpu.roll(x, 1, 0))

    def columns(r, edges):
        for v in range(-1, VECS + 1) if edges else range(VECS):
            rows = pl.ds(8 * v + 8, 8)
            ins[rows] = jnp.where(even_lane, qr[r, rows], ql[r, rows])
        for v in range(VECS):
            here, rows = pl.ds(8 * v + 8, 8), pl.ds(8 * v, 8)
            c = ins[here]
            before = ins[rows] if edges or v > 0 else c
            after = ins[pl.ds(8 * v + 16, 8)] if edges or v < VECS - 1 else c
            back = roll(jnp.where(lane >= NZ - 16, before, c), 16)
            ahead = roll(jnp.where(lane < 16, after, c), NZ - 16)
            total = c + jnp.where(sub == 0, pltpu.roll(back, 1, 0), pltpu.roll(c, 1, 0))
            total = total + jnp.where(sub == 7, pltpu.roll(ahead, 7, 0), pltpu.roll(c, 7, 0))
            up, down = roll(c, NZ - 2), roll(c, 2)
            if edges:
                above = jnp.where(even_lane, xq[r, 1, 1], xq[r, 1, 0])
                below = jnp.where(even_lane, xq[r, 0, 1], xq[r, 0, 0])
                back = (NZ - 2 * v) % NZ
                below = roll(below, back)
                up = jnp.where(group >= 14, roll(above, 14 - 2 * v), up)
                down = jnp.where(group < 2, below, down)
                xins[rows] = jnp.where(odd, roll(above, back), below)
            total = total + jnp.where(odd, up, down)
            left, right = ql[r, here] + qlo[r, rows], qr[r, here] + qhi[r, rows]
            total = total + jnp.where(even_lane, roll(right, NZ - 1), roll(left, 1))
            total = total + jnp.where(even_lane, sqr[rows], sql[rows])
            rins[rows] = total * SIXTH

    def beside(c, edge, m):
        edge = roll(edge, NZ - 1 - 2 * m)
        return jnp.where(first, edge, roll(c, 1)) + jnp.where(last, edge, roll(c, NZ - 1))

    def around(ref, lead, row, edge, m):
        c = ref[(*lead, pl.ds(row, 8))]
        total = c + ref[(*lead, pl.ds(row - 1, 8))] + ref[(*lead, pl.ds(row + 1, 8))]
        return total + beside(c, edge, m)

    def red_tile(r, q, t):
        row = TOP + 8 * t
        rows = pl.ds(row, 8)
        c = blk[r, q + 1, rows]
        total = c + jnp.where(first, 0.0, roll(c, 1)) + jnp.where(last, 0.0, roll(c, NZ - 1))
        up = jnp.where(sub == 0, 0.0, pltpu.roll(c, 1, 0)) if t == 0 else blk[r, q + 1, pl.ds(row - 1, 8)]
        down = jnp.where(sub == 7, 0.0, pltpu.roll(c, 7, 0)) if t == TILES - 1 else blk[r, q + 1, pl.ds(row + 1, 8)]
        above = blk[r, q + 2, rows] if q < NQ - 1 else 0.0
        below = blk[r, q, rows] if q > 0 else 0.0
        total = total + up + down + jnp.where(odd, above, below)
        red[q + 1, rows] = (total + sred[q + 1, rows]) * SIXTH

    def complete_z(q, t):
        rows = pl.ds(TOP + 8 * t, 8)
        edge = roll(ins[pl.ds(8 * (t // 8) + 8, 8)], NZ - 1 - 2 * slot(t, q))
        red[q + 1, rows] = red[q + 1, rows] + jnp.where(outer, edge, 0.0) * SIXTH

    def red_beyond(r, q, t):
        rows = pl.ds(TOP + 8 * t, 8)
        total = around(blk, (r, q + 1), TOP + 8 * t, ins[pl.ds(8 * (t // 8) + 8, 8)], slot(t, q))
        total = total + jnp.where(odd, blk[r, q + 2, rows], blk[r, q, rows])
        red[q + 1, rows] = (total + sred[q + 1, rows]) * SIXTH

    def complete(r, q, t):
        row = TOP + 8 * t
        rows = pl.ds(row, 8)
        more = None
        if t == 0:
            more = jnp.where(sub == 0, blk[r, q + 1, pl.ds(row - 1, 8)], 0.0)
        if t == TILES - 1:
            more = jnp.where(sub == 7, blk[r, q + 1, pl.ds(row + 1, 8)], 0.0)
        side = None
        if q == 0:
            side = jnp.where(odd, 0.0, blk[r, 0, rows])
        if q == NQ - 1:
            side = jnp.where(odd, blk[r, 9, rows], 0.0)
        if side is not None:
            more = side if more is None else more + side
        if more is not None:
            red[q + 1, rows] = red[q + 1, rows] + more * SIXTH

    def halo_tiles(r, tiles):
        for t in tiles:
            row = TOP + 8 * t
            rows = pl.ds(row, 8)
            low, high = blk[r, 0, rows], blk[r, 9, rows]
            c, far = jnp.where(odd, high, low), jnp.where(odd, low, high)
            total = jnp.where(odd, blk[r, 0, pl.ds(row - 1, 8)], blk[r, 9, pl.ds(row - 1, 8)])
            total = total + jnp.where(odd, blk[r, 0, pl.ds(row + 1, 8)], blk[r, 9, pl.ds(row + 1, 8)])
            total = total + beside(c, xins[pl.ds(8 * (t // 8), 8)], slot(t, 0))
            total = total + far + jnp.where(odd, blk[r, 1, rows], blk[r, 8, rows])
            red[0, rows] = (total + sx[pl.ds(8 * t, 8)]) * inside

    def black_tile(r, q, t, final):
        rows = pl.ds(TOP + 8 * t, 8)
        total = around(red, (q + 1,), TOP + 8 * t, rins[pl.ds(8 * (t // 8), 8)], slot(t, q))
        above = (0 if q == NQ - 1 else q + 2) if isinstance(q, int) else q + 2
        total = total + jnp.where(odd, red[q, rows], red[above, rows])
        mine = pl.ds(8 * t, 8)
        value = (total + sblk[q, mine]) * SIXTH
        if final:
            other = red[q + 1, rows]
            merged[2 * q, mine] = jnp.where(odd, value, other)
            merged[2 * q + 1, mine] = jnp.where(odd, other, value)
        else:
            blk[r + 1, q + 1, rows] = value

    def finish_ends(r, final):
        for q in range(NQ):
            for t in (-1, TILES):
                red_beyond(r, q, t)
            for t in (0, 1, TILES - 2, TILES - 1):
                complete(r, q, t)
        halo_tiles(r, (0, 1, TILES - 2, TILES - 1))
        for q in range(NQ):
            for t in ENDS:
                black_tile(r, q, t, final)

    def finish_sides(r, final, ready=None):
        for q in (0, NQ - 1):
            for t in range(2, TILES - 2):
                complete(r, q, t)
        halo_tiles(r, range(2, TILES - 2))
        for n, q in enumerate((0, NQ - 1)):
            for t in range(1, TILES - 1):
                black_tile(r, q, t, final)
            if ready is not None:
                ready(n)

    return types.SimpleNamespace(**locals())


def kernel(
    field, source,
    blk, red, sred, sblk, ql, qr, xq, qlo, qhi, sql, sqr, sx, merged,
    fld, src, elo, ehi, xe, sqlo, sqhi, ins, xins, rins, sxs, sxd,
    load_sem, send_sem, recv_sem, ssend_sem, srecv_sem,
):
    def load(array, buffer, half, n):
        planes = pl.ds(4 * n, 4)
        return pltpu.make_async_copy(array.at[planes], buffer.at[planes], load_sem.at[half, n])

    for n in range(4):
        load(field, fld, 0, n).start()

    gx, gy, gz = (lax.axis_index(a) for a in ("gx", "gy", "gz"))
    nx, ny, nz = (lax.axis_size(a) for a in ("gx", "gy", "gz"))
    low_wall, high_wall = gx == 0, gx == nx - 1

    def device(d):
        return {
            "gx": gx + d[0],
            "gy": lax.rem(gy + d[1] + ny, ny),
            "gz": lax.rem(gz + d[2] + nz, nz),
        }

    def exists(d):
        if d[0] > 0:
            return gx < nx - 1
        if d[0] < 0:
            return gx > 0
        return None

    def opposite(d):
        return tuple(-v for v in d)

    def block_slices(d):
        dx, dy, _ = d
        sp, dp = ((8, 0) if dx > 0 else (1, 9)) if dx else (pl.ds(1, NQ), pl.ds(1, NQ))
        sr, dr = ((TOP + NY - 8, TOP - 8) if dy > 0 else (TOP, TOP + NY)) if dy else (TOP, TOP)
        n = 8 if dy else NY
        return (sp, pl.ds(sr, n)), (dp, pl.ds(dr, n))

    def refs(r, d):
        dx, dy, dz = d
        if dz == 0:
            s, t = block_slices(d)
            return blk.at[(r, *s)], blk.at[(r, *t)]
        col, dst = (qhi, ql) if dz > 0 else (qlo, qr)
        own = pl.ds(8, COLS)
        if dx:
            place = (r, 0 if dx > 0 else 1, 0 if dz > 0 else 1)
            return xe.at[place], xq.at[place]
        if dy:
            end, dr = (1, 0) if dy > 0 else (0, COLS + 8)
            return (ehi if dz > 0 else elo).at[r, end], dst.at[r, pl.ds(dr, 8)]
        return col.at[r], dst.at[r, own]

    def side(d):
        return 1 if d[0] > 0 else 2 if d[0] < 0 else 0

    def message(r, m):
        d = MESSAGES[m]
        s, t = refs(r, d)
        group = 3 if d in Z_FACES else side(d)
        return pltpu.make_async_remote_copy(
            src_ref=s, dst_ref=t, send_sem=send_sem.at[side(d)], recv_sem=recv_sem.at[r, group],
            device_id=device(d), device_id_type=MESH,
        )

    def smessage(m):
        d = FACES[m]
        if d[2]:
            s, t = (sqhi, sql) if d[2] > 0 else (sqlo, sqr)
        elif d[0]:
            n = side(d) - 1
            s, t = sxs.at[n], sxd.at[n]
        else:
            s, t = block_slices(d)
            s, t = sred.at[s], sred.at[t]
        group = 3 if d in Z_FACES else side(d)
        return pltpu.make_async_remote_copy(
            src_ref=s, dst_ref=t, send_sem=ssend_sem.at[side(d)], recv_sem=srecv_sem.at[group],
            device_id=device(d), device_id_type=MESH,
        )

    def start(make, dirs, select):
        for m, d in enumerate(dirs):
            if d in select:
                when(exists(d), lambda m=m: make(m).start())

    def wait(sem, kib):
        some = fld.at[pl.ds(0, 2), pl.ds(0, kib)]
        pltpu.make_async_copy(some, some, sem).wait()

    SIDE_KIB = 128 + 4 * 4

    def wait_sides(sems, kib, sent):
        when(exists((1 if sent else -1, 0, 0)), lambda: wait(sems(1), kib))
        when(exists((-1 if sent else 1, 0, 0)), lambda: wait(sems(2), kib))

    def arrived_z(r):
        wait(recv_sem.at[r, 3], 2 * 16)

    def arrived_rest(r):
        wait(recv_sem.at[r, 0], 4 * 4 + 2 * 32)
        wait_sides(lambda g: recv_sem.at[r, g], SIDE_KIB, False)

    def sent():
        wait(send_sem.at[0], 4 * 4 + 2 * 16 + 2 * 32)
        wait_sides(lambda g: send_sem.at[g], SIDE_KIB, True)

    def ssent():
        wait(ssend_sem.at[0], 2 * 16 + 2 * 32)
        wait_sides(lambda g: ssend_sem.at[g], 64, True)

    barrier = pltpu.get_barrier_semaphore()
    for d in MESSAGES:
        when(exists(d), lambda d=d: pl.semaphore_signal(barrier, inc=1, device_id=device(d), device_id_type=MESH))

    w = cells(blk, red, sred, sblk, ql, qr, xq, qlo, qhi, sql, sqr, sx, merged, ins, xins, rins)
    sub, odd, half, half_after = w.sub, w.odd, w.half, w.half_after
    roll, slot, swap = w.roll, w.slot, w.swap

    def collect(lo, hi, lead, t, q, value, rows=None):
        m = slot(t, q)
        turned = roll(value, jnp.bitwise_and(2 * m + 2, NZ - 1))
        rows = pl.ds(8 * (t // 8), 8) if rows is None else rows
        hi[(*lead, rows)] = jnp.where(half == m, turned, hi[(*lead, rows)])
        lo[(*lead, rows)] = jnp.where(half_after == m, turned, lo[(*lead, rows)])

    def collect_edges(r):
        for end, t in enumerate(ENDS):
            for q in range(NQ):
                collect(elo, ehi, (r, end), t, q, blk[r, q + 1, pl.ds(TOP + 8 * t, 8)], pl.ds(0, 8))
            elo[r, end] = roll(elo[r, end], NZ - 2)

    def settle(lo, lead):
        for v in range(VECS):
            rows = pl.ds(8 * v, 8)
            lo[(*lead, rows)] = roll(lo[(*lead, rows)], NZ - 2)

    def collect_xz(r):
        for place, pair in enumerate((NQ - 1, 0)):
            for z, col in enumerate((qhi, qlo)):
                piece = roll(col[r, pl.ds(0, 8)], (NZ - 2 * pair) % NZ)
                for v in range(1, VECS):
                    more = roll(col[r, pl.ds(8 * v, 8)], (2 * v - 2 * pair) % NZ)
                    piece = jnp.where(jnp.right_shift(w.group, 1) == v, more, piece)
                xe[r, place, z] = piece

    zero = jnp.zeros((ROWS, NZ), jnp.float32)

    def wall(pair, plane):
        for r in range(SWEEPS):
            blk[r, pair] = zero
            for z in range(2):
                xq[r, plane, z] = jnp.zeros((8, NZ), jnp.float32)
        sxd[0 if pair == 0 else 1] = jnp.zeros((NY // 2, NZ), jnp.float32)

    pl.when(low_wall)(lambda: wall(0, 0))
    pl.when(high_wall)(lambda: wall(9, 1))
    def pack_field(q, c):
        for t in range(TILES):
            rows = pl.ds(8 * t, 8)
            value = jnp.where(odd, fld[2 * q, rows], fld[2 * q + 1, rows])
            blk[0, q + 1, pl.ds(TOP + 8 * t, 8)] = value
            collect(qlo, qhi, (0,), t, q, value)
        return c

    def packed_field(n, c):
        load(field, fld, 0, n).wait()
        load(source, src, 1, n).start()
        return pack_field(2 * n + 1, pack_field(2 * n, c))

    lax.fori_loop(0, 4, packed_field, 0)
    collect_edges(0)
    settle(qlo, (0,))
    collect_xz(0)

    walls = jnp.where(jnp.logical_or(low_wall, high_wall), 1, 0)
    pl.semaphore_wait(barrier, len(MESSAGES) - 5 * walls)
    start(functools.partial(message, 0), MESSAGES, EDGES + Z_FACES + Y_FACES)

    def pack_source(q, c):
        for t in range(TILES):
            rows = pl.ds(8 * t, 8)
            even_plane, odd_plane = src[2 * q, rows], src[2 * q + 1, rows]
            value = jnp.where(odd, odd_plane, even_plane)
            sred[q + 1, pl.ds(TOP + 8 * t, 8)] = value
            sblk[q, rows] = jnp.where(odd, even_plane, odd_plane)
            collect(sqlo, sqhi, (), t, q, value)
        return c

    def packed_source(n, c):
        load(source, src, 1, n).wait()
        return pack_source(2 * n + 1, pack_source(2 * n, c))

    lax.fori_loop(0, 4, packed_source, 0)
    settle(sqlo, ())
    start(smessage, FACES, Z_FACES + Y_FACES)
    start(functools.partial(message, 0), MESSAGES, X_FACES)
    for t in range(TILES // 2):
        near, away = pl.ds(TOP + 8 * t, 8), pl.ds(TOP + 8 * t + NY // 2, 8)
        sxs[0, pl.ds(8 * t, 8)] = jnp.where(odd, sred[NQ, near], swap(sred[NQ, away]))
        sxs[1, pl.ds(8 * t, 8)] = jnp.where(odd, swap(sred[1, away]), sred[1, near])
    start(smessage, FACES, X_FACES)

    def sweep(r, final):
        for q in range(NQ):
            for t in range(TILES):
                w.red_tile(r, q, t)
        arrived_z(r)
        pl.when(r == 0)(lambda: wait(srecv_sem.at[3], 2 * 16))

        w.columns(r, False)

        for q in range(NQ):
            for t in range(TILES):
                w.complete_z(q, t)

        def black_inner(n, c):
            for q in (3 * n + 1, 3 * n + 2, 3 * n + 3):
                for t in range(1, TILES - 1):
                    w.black_tile(r, q, t, final)
            return c

        black_inner(0, 0)
        black_inner(1, 0)
        if not final:
            for t in range(1, TILES - 1):
                for q in range(1, NQ - 1):
                    collect(qlo, qhi, (r + 1,), t, q, blk[r + 1, q + 1, pl.ds(TOP + 8 * t, 8)])

        arrived_rest(r)

        @pl.when(r == 0)
        def _():
            wait(srecv_sem.at[0], 2 * 32)
            wait_sides(lambda g: srecv_sem.at[g], 64, False)
            for t in range(TILES // 2):
                low, high = sxd[0, pl.ds(8 * t, 8)], sxd[1, pl.ds(8 * t, 8)]
                sx[pl.ds(8 * t, 8)] = jnp.where(odd, low, high)
                sx[pl.ds(8 * t + NY // 2, 8)] = swap(jnp.where(odd, high, low))

        sent()
        if final:
            return
        w.columns(r, True)
        w.finish_ends(r, False)
        after = functools.partial(message, r + 1)
        collect_edges(r + 1)
        start(after, MESSAGES, YZ_EDGES + XY_EDGES + Y_FACES)
        w.finish_sides(r, False)
        for t in range(TILES):
            for q in range(NQ) if t in ENDS else (0, NQ - 1):
                collect(qlo, qhi, (r + 1,), t, q, blk[r + 1, q + 1, pl.ds(TOP + 8 * t, 8)])
        settle(qlo, (r + 1,))
        start(after, MESSAGES, Z_FACES)
        collect_xz(r + 1)
        start(after, MESSAGES, XZ_EDGES + X_FACES)

    def sweeps(r, c):
        sweep(r, False)
        return c

    lax.fori_loop(0, SWEEPS - 1, sweeps, 0)
    sweep(SWEEPS - 1, True)
    ssent()


def finish(
    blk, red_in, sred, sblk, ql, qr, xq, qlo, qhi, sql, sqr, sx, merged, out, red,
    late, ins, xins, rins, sem,
):
    del red_in
    w = cells(blk, red, sred, sblk, ql, qr, xq, qlo, qhi, sql, sqr, sx, late, ins, xins, rins)

    def store(n):
        planes, rows = [
            (pl.ds(2, 2 * NQ - 4), pl.ds(8, NY - 16)),
            (pl.ds(2, 2 * NQ - 4), pl.ds(0, 8)),
            (pl.ds(2, 2 * NQ - 4), pl.ds(NY - 8, 8)),
            (pl.ds(0, 2), pl.ds(0, NY)),
            (pl.ds(2 * NQ - 2, 2), pl.ds(0, NY)),
        ][n]
        origin = merged if n == 0 else late
        return pltpu.make_async_copy(origin.at[planes, rows], out.at[planes, rows], sem.at[n])

    store(0).start()
    r = SWEEPS - 1
    w.columns(r, True)
    w.finish_ends(r, True)
    store(1).start()
    store(2).start()
    w.finish_sides(r, True, lambda n: store(3 + n).start())
    for n in range(5):
        store(n).wait()


def on_device(field, source):
    f32 = jnp.float32
    dma = pltpu.SemaphoreType.DMA
    columns = (COLS, NZ)
    shared = [
        (SWEEPS, NQ + 2, ROWS, NZ),
        (NQ + 1, ROWS, NZ),
        (NQ + 2, ROWS, NZ),
        (NQ, NY, NZ),
        (SWEEPS, COLS + 16, NZ),
        (SWEEPS, COLS + 16, NZ),
        (SWEEPS, 2, 2, 8, NZ),
        (SWEEPS, *columns),
        (SWEEPS, *columns),
        columns,
        columns,
        (NY, NZ),
        (2 * NQ, NY, NZ),
    ]
    vmem, hbm = (pl.BlockSpec(memory_space=m) for m in (pltpu.VMEM, pltpu.HBM))
    inserts = [pltpu.VMEM(shape, f32) for shape in ((COLS + 16, NZ), columns, columns)]
    field, source = (pltpu.with_memory_space_constraint(x, pltpu.HBM) for x in (field, source))
    state = pl.pallas_call(
        kernel,
        name="smooth",
        out_shape=[pltpu.VMEM(shape, f32) for shape in shared],
        in_specs=[hbm] * 2,
        out_specs=[vmem] * len(shared),
        scratch_shapes=[
            pltpu.VMEM((2 * NQ, NY, NZ), f32),
            pltpu.VMEM((2 * NQ, NY, NZ), f32),
            pltpu.VMEM((SWEEPS, 2, 8, NZ), f32),
            pltpu.VMEM((SWEEPS, 2, 8, NZ), f32),
            pltpu.VMEM((SWEEPS, 2, 2, 8, NZ), f32),
            pltpu.VMEM(columns, f32),
            pltpu.VMEM(columns, f32),
            *inserts,
            pltpu.VMEM((2, NY // 2, NZ), f32),
            pltpu.VMEM((2, NY // 2, NZ), f32),
            dma((2, 4)),
            dma((3,)),
            dma((SWEEPS, 4)),
            dma((3,)),
            dma((4,)),
        ],
        compiler_params=pltpu.CompilerParams(
            collective_id=0, has_side_effects=True, vmem_limit_bytes=VMEM_GRANT
        ),
    )(field, source)
    state = [pltpu.with_memory_space_constraint(x, pltpu.VMEM) for x in state]
    result, _ = pl.pallas_call(
        finish,
        name="finish",
        out_shape=[jax.ShapeDtypeStruct(field.shape, f32), pltpu.VMEM(shared[1], f32)],
        in_specs=[vmem] * len(shared),
        out_specs=[hbm, vmem],
        input_output_aliases={1: 1},
        scratch_shapes=[pltpu.VMEM((2 * NQ, NY, NZ), f32), *inserts, dma((5,))],
        compiler_params=pltpu.CompilerParams(vmem_limit_bytes=VMEM_GRANT),
    )(*state)
    return result


def solution(mesh):
    spec = P("gx", "gy", "gz")
    return jax.shard_map(
        on_device, mesh=mesh, in_specs=(spec, spec), out_specs=spec, check_vma=False
    )
```

```python
import functools
import itertools
import types

import jax
import jax.numpy as jnp
from jax import lax
from jax.experimental import pallas as pl
from jax.experimental.pallas import tpu as pltpu
from jax.sharding import PartitionSpec as P

MESH = pl.DeviceIdType.MESH
SWEEPS = 3
NQ, NY, NZ = 8, 256, 128
TILES = NY // 8
ENDS = (0, TILES - 1)
TOP = 16
ROWS = NY + 2 * TOP
VECS = TILES // 8
COLS = 8 * VECS
SIXTH = 1.0 / 6.0
VMEM_GRANT = 24 << 20

EDGES = [d for d in itertools.product((-1, 0, 1), repeat=3) if sum(map(abs, d)) == 2]
FACES = [(0, 0, 1), (0, 0, -1), (0, 1, 0), (0, -1, 0), (1, 0, 0), (-1, 0, 0)]
MESSAGES = [d for d in EDGES if d[0] == 0] + [d for d in EDGES if d[0]] + FACES
X_FACES, Y_FACES, Z_FACES = FACES[4:], FACES[2:4], FACES[:2]
YZ_EDGES, XY_EDGES, XZ_EDGES = ([d for d in EDGES if d[a] == 0] for a in (0, 2, 1))


def when(cond, f):
    if cond is None:
        f()
    else:
        pl.when(cond)(f)


def cells(blk, red, sred, sblk, ql, qr, xq, qlo, qhi, sql, sqr, sx, merged, ins, xins, rins):
    gx = lax.axis_index("gx")
    low_wall, high_wall = gx == 0, gx == lax.axis_size("gx") - 1
    lane = lax.broadcasted_iota(jnp.int32, (8, NZ), 1)
    sub = lax.broadcasted_iota(jnp.int32, (8, NZ), 0)
    odd = jnp.bitwise_and(lane + sub, 1) == 1
    even_lane = jnp.bitwise_and(lane, 1) == 0
    first, last = lane == 0, lane == NZ - 1
    outer = jnp.logical_or(first, last)
    group = jnp.bitwise_and(lane, 15)
    half = jnp.right_shift(lane, 1)
    half_after = jnp.bitwise_and(half - 1, NZ // 2 - 1)

    def roll(x, shift):
        return pltpu.roll(x, shift, 1)

    def slot(t, q):
        return 8 * (t % 8) + q

    inside = jnp.where(odd, jnp.where(low_wall, 0.0, SIXTH), jnp.where(high_wall, 0.0, SIXTH))

    def swap(x):
        return jnp.where(jnp.bitwise_and(sub, 1) == 0, pltpu.roll(x, 7, 0), pltpu.roll(x, 1, 0))

    def columns(r, edges):
        for v in range(-1, VECS + 1) if edges else range(VECS):
            rows = pl.ds(8 * v + 8, 8)
            ins[rows] = jnp.where(even_lane, qr[r, rows], ql[r, rows])
        for v in range(VECS):
            here, rows = pl.ds(8 * v + 8, 8), pl.ds(8 * v, 8)
            c = ins[here]
            before = ins[rows] if edges or v > 0 else c
            after = ins[pl.ds(8 * v + 16, 8)] if edges or v < VECS - 1 else c
            back = roll(jnp.where(lane >= NZ - 16, before, c), 16)
            ahead = roll(jnp.where(lane < 16, after, c), NZ - 16)
            total = c + jnp.where(sub == 0, pltpu.roll(back, 1, 0), pltpu.roll(c, 1, 0))
            total = total + jnp.where(sub == 7, pltpu.roll(ahead, 7, 0), pltpu.roll(c, 7, 0))
            up, down = roll(c, NZ - 2), roll(c, 2)
            if edges:
                above = jnp.where(even_lane, xq[r, 1, 1], xq[r, 1, 0])
                below = jnp.where(even_lane, xq[r, 0, 1], xq[r, 0, 0])
                back = (NZ - 2 * v) % NZ
                below = roll(below, back)
                up = jnp.where(group >= 14, roll(above, 14 - 2 * v), up)
                down = jnp.where(group < 2, below, down)
                xins[rows] = jnp.where(odd, roll(above, back), below)
            total = total + jnp.where(odd, up, down)
            left, right = ql[r, here] + qlo[r, rows], qr[r, here] + qhi[r, rows]
            total = total + jnp.where(even_lane, roll(right, NZ - 1), roll(left, 1))
            total = total + jnp.where(even_lane, sqr[rows], sql[rows])
            rins[rows] = total * SIXTH

    def beside(c, edge, m):
        edge = roll(edge, NZ - 1 - 2 * m)
        return jnp.where(first, edge, roll(c, 1)) + jnp.where(last, edge, roll(c, NZ - 1))

    def around(ref, lead, row, edge, m):
        c = ref[(*lead, pl.ds(row, 8))]
        total = c + ref[(*lead, pl.ds(row - 1, 8))] + ref[(*lead, pl.ds(row + 1, 8))]
        return total + beside(c, edge, m)

    def red_tile(r, q, t):
        row = TOP + 8 * t
        rows = pl.ds(row, 8)
        c = blk[r, q + 1, rows]
        total = c + jnp.where(first, 0.0, roll(c, 1)) + jnp.where(last, 0.0, roll(c, NZ - 1))
        up = jnp.where(sub == 0, 0.0, pltpu.roll(c, 1, 0)) if t == 0 else blk[r, q + 1, pl.ds(row - 1, 8)]
        down = jnp.where(sub == 7, 0.0, pltpu.roll(c, 7, 0)) if t == TILES - 1 else blk[r, q + 1, pl.ds(row + 1, 8)]
        above = blk[r, q + 2, rows] if q < NQ - 1 else 0.0
        below = blk[r, q, rows] if q > 0 else 0.0
        total = total + up + down + jnp.where(odd, above, below)
        red[q + 1, rows] = (total + sred[q + 1, rows]) * SIXTH

    def complete_z(q, t):
        rows = pl.ds(TOP + 8 * t, 8)
        edge = roll(ins[pl.ds(8 * (t // 8) + 8, 8)], NZ - 1 - 2 * slot(t, q))
        red[q + 1, rows] = red[q + 1, rows] + jnp.where(outer, edge, 0.0) * SIXTH

    def red_beyond(r, q, t):
        rows = pl.ds(TOP + 8 * t, 8)
        total = around(blk, (r, q + 1), TOP + 8 * t, ins[pl.ds(8 * (t // 8) + 8, 8)], slot(t, q))
        total = total + jnp.where(odd, blk[r, q + 2, rows], blk[r, q, rows])
        red[q + 1, rows] = (total + sred[q + 1, rows]) * SIXTH

    def complete(r, q, t):
        row = TOP + 8 * t
        rows = pl.ds(row, 8)
        more = None
        if t == 0:
            more = jnp.where(sub == 0, blk[r, q + 1, pl.ds(row - 1, 8)], 0.0)
        if t == TILES - 1:
            more = jnp.where(sub == 7, blk[r, q + 1, pl.ds(row + 1, 8)], 0.0)
        side = None
        if q == 0:
            side = jnp.where(odd, 0.0, blk[r, 0, rows])
        if q == NQ - 1:
            side = jnp.where(odd, blk[r, 9, rows], 0.0)
        if side is not None:
            more = side if more is None else more + side
        if more is not None:
            red[q + 1, rows] = red[q + 1, rows] + more * SIXTH

    def halo_tiles(r, tiles):
        for t in tiles:
            row = TOP + 8 * t
            rows = pl.ds(row, 8)
            low, high = blk[r, 0, rows], blk[r, 9, rows]
            c, far = jnp.where(odd, high, low), jnp.where(odd, low, high)
            total = jnp.where(odd, blk[r, 0, pl.ds(row - 1, 8)], blk[r, 9, pl.ds(row - 1, 8)])
            total = total + jnp.where(odd, blk[r, 0, pl.ds(row + 1, 8)], blk[r, 9, pl.ds(row + 1, 8)])
            total = total + beside(c, xins[pl.ds(8 * (t // 8), 8)], slot(t, 0))
            total = total + far + jnp.where(odd, blk[r, 1, rows], blk[r, 8, rows])
            red[0, rows] = (total + sx[pl.ds(8 * t, 8)]) * inside

    def black_tile(r, q, t, final):
        rows = pl.ds(TOP + 8 * t, 8)
        total = around(red, (q + 1,), TOP + 8 * t, rins[pl.ds(8 * (t // 8), 8)], slot(t, q))
        above = (0 if q == NQ - 1 else q + 2) if isinstance(q, int) else q + 2
        total = total + jnp.where(odd, red[q, rows], red[above, rows])
        mine = pl.ds(8 * t, 8)
        value = (total + sblk[q, mine]) * SIXTH
        if final:
            other = red[q + 1, rows]
            merged[2 * q, mine] = jnp.where(odd, value, other)
            merged[2 * q + 1, mine] = jnp.where(odd, other, value)
        else:
            blk[r + 1, q + 1, rows] = value

    def finish_ends(r, final):
        for q in range(NQ):
            for t in (-1, TILES):
                red_beyond(r, q, t)
            for t in (0, 1, TILES - 2, TILES - 1):
                complete(r, q, t)
        halo_tiles(r, (0, 1, TILES - 2, TILES - 1))
        for q in range(NQ):
            for t in ENDS:
                black_tile(r, q, t, final)

    def finish_sides(r, final, ready=None):
        for q in (0, NQ - 1):
            for t in range(2, TILES - 2):
                complete(r, q, t)
        halo_tiles(r, range(2, TILES - 2))
        for n, q in enumerate((0, NQ - 1)):
            for t in range(1, TILES - 1):
                black_tile(r, q, t, final)
            if ready is not None:
                ready(n)

    return types.SimpleNamespace(**locals())


def kernel(
    field, source,
    blk, red, sred, sblk, ql, qr, xq, qlo, qhi, sql, sqr, sx, merged,
    fld, src, elo, ehi, xe, sqlo, sqhi, ins, xins, rins, sxs, sxd,
    load_sem, send_sem, recv_sem, ssend_sem, srecv_sem,
):
    def load(array, buffer, half, n):
        planes = pl.ds(4 * n, 4)
        return pltpu.make_async_copy(array.at[planes], buffer.at[planes], load_sem.at[half, n])

    for n in range(4):
        load(field, fld, 0, n).start()
    for n in range(4):
        load(source, src, 1, n).start()

    gx, gy, gz = (lax.axis_index(a) for a in ("gx", "gy", "gz"))
    nx, ny, nz = (lax.axis_size(a) for a in ("gx", "gy", "gz"))
    low_wall, high_wall = gx == 0, gx == nx - 1

    def device(d):
        return {
            "gx": gx + d[0],
            "gy": lax.rem(gy + d[1] + ny, ny),
            "gz": lax.rem(gz + d[2] + nz, nz),
        }

    def exists(d):
        if d[0] > 0:
            return gx < nx - 1
        if d[0] < 0:
            return gx > 0
        return None

    def opposite(d):
        return tuple(-v for v in d)

    def block_slices(d):
        dx, dy, _ = d
        sp, dp = ((8, 0) if dx > 0 else (1, 9)) if dx else (pl.ds(1, NQ), pl.ds(1, NQ))
        sr, dr = ((TOP + NY - 8, TOP - 8) if dy > 0 else (TOP, TOP + NY)) if dy else (TOP, TOP)
        n = 8 if dy else NY
        return (sp, pl.ds(sr, n)), (dp, pl.ds(dr, n))

    def refs(r, d):
        dx, dy, dz = d
        if dz == 0:
            s, t = block_slices(d)
            return blk.at[(r, *s)], blk.at[(r, *t)]
        col, dst = (qhi, ql) if dz > 0 else (qlo, qr)
        own = pl.ds(8, COLS)
        if dx:
            place = (r, 0 if dx > 0 else 1, 0 if dz > 0 else 1)
            return xe.at[place], xq.at[place]
        if dy:
            end, dr = (1, 0) if dy > 0 else (0, COLS + 8)
            return (ehi if dz > 0 else elo).at[r, end], dst.at[r, pl.ds(dr, 8)]
        return col.at[r], dst.at[r, own]

    def side(d):
        return 1 if d[0] > 0 else 2 if d[0] < 0 else 0

    def message(r, m):
        d = MESSAGES[m]
        s, t = refs(r, d)
        group = 3 if d in Z_FACES else side(d)
        return pltpu.make_async_remote_copy(
            src_ref=s, dst_ref=t, send_sem=send_sem.at[side(d)], recv_sem=recv_sem.at[r, group],
            device_id=device(d), device_id_type=MESH,
        )

    def smessage(m):
        d = FACES[m]
        if d[2]:
            s, t = (sqhi, sql) if d[2] > 0 else (sqlo, sqr)
        elif d[0]:
            n = side(d) - 1
            s, t = sxs.at[n], sxd.at[n]
        else:
            s, t = block_slices(d)
            s, t = sred.at[s], sred.at[t]
        group = 3 if d in Z_FACES else side(d)
        return pltpu.make_async_remote_copy(
            src_ref=s, dst_ref=t, send_sem=ssend_sem.at[side(d)], recv_sem=srecv_sem.at[group],
            device_id=device(d), device_id_type=MESH,
        )

    def start(make, dirs, select):
        for m, d in enumerate(dirs):
            if d in select:
                when(exists(d), lambda m=m: make(m).start())

    def wait(sem, kib):
        some = fld.at[pl.ds(0, 2), pl.ds(0, kib)]
        pltpu.make_async_copy(some, some, sem).wait()

    SIDE_KIB = 128 + 4 * 4

    def wait_sides(sems, kib, sent):
        when(exists((1 if sent else -1, 0, 0)), lambda: wait(sems(1), kib))
        when(exists((-1 if sent else 1, 0, 0)), lambda: wait(sems(2), kib))

    def arrived_z(r):
        wait(recv_sem.at[r, 3], 2 * 16)

    def arrived_rest(r):
        wait(recv_sem.at[r, 0], 4 * 4 + 2 * 32)
        wait_sides(lambda g: recv_sem.at[r, g], SIDE_KIB, False)

    def sent():
        wait(send_sem.at[0], 4 * 4 + 2 * 16 + 2 * 32)
        wait_sides(lambda g: send_sem.at[g], SIDE_KIB, True)

    def ssent():
        wait(ssend_sem.at[0], 2 * 16 + 2 * 32)
        wait_sides(lambda g: ssend_sem.at[g], 64, True)

    barrier = pltpu.get_barrier_semaphore()
    for d in MESSAGES:
        when(exists(d), lambda d=d: pl.semaphore_signal(barrier, inc=1, device_id=device(d), device_id_type=MESH))

    w = cells(blk, red, sred, sblk, ql, qr, xq, qlo, qhi, sql, sqr, sx, merged, ins, xins, rins)
    sub, odd, half, half_after = w.sub, w.odd, w.half, w.half_after
    roll, slot, swap = w.roll, w.slot, w.swap

    def collect(lo, hi, lead, t, q, value, rows=None):
        m = slot(t, q)
        turned = roll(value, jnp.bitwise_and(2 * m + 2, NZ - 1))
        rows = pl.ds(8 * (t // 8), 8) if rows is None else rows
        hi[(*lead, rows)] = jnp.where(half == m, turned, hi[(*lead, rows)])
        lo[(*lead, rows)] = jnp.where(half_after == m, turned, lo[(*lead, rows)])

    def collect_edges(r):
        for end, t in enumerate(ENDS):
            for q in range(NQ):
                collect(elo, ehi, (r, end), t, q, blk[r, q + 1, pl.ds(TOP + 8 * t, 8)], pl.ds(0, 8))
            elo[r, end] = roll(elo[r, end], NZ - 2)

    def settle(lo, lead):
        for v in range(VECS):
            rows = pl.ds(8 * v, 8)
            lo[(*lead, rows)] = roll(lo[(*lead, rows)], NZ - 2)

    def collect_xz(r):
        for place, pair in enumerate((NQ - 1, 0)):
            for z, col in enumerate((qhi, qlo)):
                piece = roll(col[r, pl.ds(0, 8)], (NZ - 2 * pair) % NZ)
                for v in range(1, VECS):
                    more = roll(col[r, pl.ds(8 * v, 8)], (2 * v - 2 * pair) % NZ)
                    piece = jnp.where(jnp.right_shift(w.group, 1) == v, more, piece)
                xe[r, place, z] = piece

    zero = jnp.zeros((ROWS, NZ), jnp.float32)

    def wall(pair, plane):
        for r in range(SWEEPS):
            blk[r, pair] = zero
            for z in range(2):
                xq[r, plane, z] = jnp.zeros((8, NZ), jnp.float32)
        sxd[0 if pair == 0 else 1] = jnp.zeros((NY // 2, NZ), jnp.float32)

    pl.when(low_wall)(lambda: wall(0, 0))
    pl.when(high_wall)(lambda: wall(9, 1))
    def pack_field(q, c):
        for t in range(TILES):
            rows = pl.ds(8 * t, 8)
            value = jnp.where(odd, fld[2 * q, rows], fld[2 * q + 1, rows])
            blk[0, q + 1, pl.ds(TOP + 8 * t, 8)] = value
            collect(qlo, qhi, (0,), t, q, value)
        return c

    def packed_field(n, c):
        load(field, fld, 0, n).wait()
        return pack_field(2 * n + 1, pack_field(2 * n, c))

    for n in range(4):
        packed_field(n, 0)
    collect_edges(0)
    settle(qlo, (0,))
    collect_xz(0)

    walls = jnp.where(jnp.logical_or(low_wall, high_wall), 1, 0)
    pl.semaphore_wait(barrier, len(MESSAGES) - 5 * walls)
    start(functools.partial(message, 0), MESSAGES, EDGES + Z_FACES + Y_FACES)

    def pack_source(q, c):
        for t in range(TILES):
            rows = pl.ds(8 * t, 8)
            even_plane, odd_plane = src[2 * q, rows], src[2 * q + 1, rows]
            value = jnp.where(odd, odd_plane, even_plane)
            sred[q + 1, pl.ds(TOP + 8 * t, 8)] = value
            sblk[q, rows] = jnp.where(odd, even_plane, odd_plane)
            collect(sqlo, sqhi, (), t, q, value)
        return c

    def packed_source(n, c):
        load(source, src, 1, n).wait()
        return pack_source(2 * n + 1, pack_source(2 * n, c))

    for n in range(4):
        packed_source(n, 0)
    settle(sqlo, ())
    start(smessage, FACES, Z_FACES + Y_FACES)
    start(functools.partial(message, 0), MESSAGES, X_FACES)
    for t in range(TILES // 2):
        near, away = pl.ds(TOP + 8 * t, 8), pl.ds(TOP + 8 * t + NY // 2, 8)
        sxs[0, pl.ds(8 * t, 8)] = jnp.where(odd, sred[NQ, near], swap(sred[NQ, away]))
        sxs[1, pl.ds(8 * t, 8)] = jnp.where(odd, swap(sred[1, away]), sred[1, near])
    start(smessage, FACES, X_FACES)

    def sweep(r, final):
        for q in range(NQ):
            for t in range(TILES):
                w.red_tile(r, q, t)
        arrived_z(r)
        pl.when(r == 0)(lambda: wait(srecv_sem.at[3], 2 * 16))

        w.columns(r, False)

        for q in range(NQ):
            for t in range(TILES):
                w.complete_z(q, t)

        def black_inner(n, c):
            for q in (3 * n + 1, 3 * n + 2, 3 * n + 3):
                for t in range(1, TILES - 1):
                    w.black_tile(r, q, t, final)
            return c

        black_inner(0, 0)
        black_inner(1, 0)
        if not final:
            for t in range(1, TILES - 1):
                for q in range(1, NQ - 1):
                    collect(qlo, qhi, (r + 1,), t, q, blk[r + 1, q + 1, pl.ds(TOP + 8 * t, 8)])

        arrived_rest(r)

        @pl.when(r == 0)
        def _():
            wait(srecv_sem.at[0], 2 * 32)
            wait_sides(lambda g: srecv_sem.at[g], 64, False)
            for t in range(TILES // 2):
                low, high = sxd[0, pl.ds(8 * t, 8)], sxd[1, pl.ds(8 * t, 8)]
                sx[pl.ds(8 * t, 8)] = jnp.where(odd, low, high)
                sx[pl.ds(8 * t + NY // 2, 8)] = swap(jnp.where(odd, high, low))

        sent()
        if final:
            return
        w.columns(r, True)
        w.finish_ends(r, False)
        after = functools.partial(message, r + 1)
        collect_edges(r + 1)
        start(after, MESSAGES, YZ_EDGES + XY_EDGES + Y_FACES)
        w.finish_sides(r, False)
        for t in range(TILES):
            for q in range(NQ) if t in ENDS else (0, NQ - 1):
                collect(qlo, qhi, (r + 1,), t, q, blk[r + 1, q + 1, pl.ds(TOP + 8 * t, 8)])
        settle(qlo, (r + 1,))
        start(after, MESSAGES, Z_FACES)
        collect_xz(r + 1)
        start(after, MESSAGES, XZ_EDGES + X_FACES)

    def sweeps(r, c):
        sweep(r, False)
        return c

    lax.fori_loop(0, SWEEPS - 1, sweeps, 0)
    sweep(SWEEPS - 1, True)
    ssent()


def finish(
    blk, red_in, sred, sblk, ql, qr, xq, qlo, qhi, sql, sqr, sx, merged, out, red,
    late, ins, xins, rins, sem,
):
    del red_in
    w = cells(blk, red, sred, sblk, ql, qr, xq, qlo, qhi, sql, sqr, sx, late, ins, xins, rins)

    def store(n):
        planes, rows = [
            (pl.ds(2, 2 * NQ - 4), pl.ds(8, NY - 16)),
            (pl.ds(2, 2 * NQ - 4), pl.ds(0, 8)),
            (pl.ds(2, 2 * NQ - 4), pl.ds(NY - 8, 8)),
            (pl.ds(0, 2), pl.ds(0, NY)),
            (pl.ds(2 * NQ - 2, 2), pl.ds(0, NY)),
        ][n]
        origin = merged if n == 0 else late
        return pltpu.make_async_copy(origin.at[planes, rows], out.at[planes, rows], sem.at[n])

    store(0).start()
    r = SWEEPS - 1
    w.columns(r, True)
    w.finish_ends(r, True)
    store(1).start()
    store(2).start()
    w.finish_sides(r, True, lambda n: store(3 + n).start())
    for n in range(5):
        store(n).wait()


def on_device(field, source):
    f32 = jnp.float32
    dma = pltpu.SemaphoreType.DMA
    columns = (COLS, NZ)
    shared = [
        (SWEEPS, NQ + 2, ROWS, NZ),
        (NQ + 1, ROWS, NZ),
        (NQ + 2, ROWS, NZ),
        (NQ, NY, NZ),
        (SWEEPS, COLS + 16, NZ),
        (SWEEPS, COLS + 16, NZ),
        (SWEEPS, 2, 2, 8, NZ),
        (SWEEPS, *columns),
        (SWEEPS, *columns),
        columns,
        columns,
        (NY, NZ),
        (2 * NQ, NY, NZ),
    ]
    vmem, hbm = (pl.BlockSpec(memory_space=m) for m in (pltpu.VMEM, pltpu.HBM))
    inserts = [pltpu.VMEM(shape, f32) for shape in ((COLS + 16, NZ), columns, columns)]
    field, source = (pltpu.with_memory_space_constraint(x, pltpu.HBM) for x in (field, source))
    state = pl.pallas_call(
        kernel,
        name="smooth",
        out_shape=[pltpu.VMEM(shape, f32) for shape in shared],
        in_specs=[hbm] * 2,
        out_specs=[vmem] * len(shared),
        scratch_shapes=[
            pltpu.VMEM((2 * NQ, NY, NZ), f32),
            pltpu.VMEM((2 * NQ, NY, NZ), f32),
            pltpu.VMEM((SWEEPS, 2, 8, NZ), f32),
            pltpu.VMEM((SWEEPS, 2, 8, NZ), f32),
            pltpu.VMEM((SWEEPS, 2, 2, 8, NZ), f32),
            pltpu.VMEM(columns, f32),
            pltpu.VMEM(columns, f32),
            *inserts,
            pltpu.VMEM((2, NY // 2, NZ), f32),
            pltpu.VMEM((2, NY // 2, NZ), f32),
            dma((2, 4)),
            dma((3,)),
            dma((SWEEPS, 4)),
            dma((3,)),
            dma((4,)),
        ],
        compiler_params=pltpu.CompilerParams(
            collective_id=0, has_side_effects=True, vmem_limit_bytes=VMEM_GRANT
        ),
    )(field, source)
    state = [pltpu.with_memory_space_constraint(x, pltpu.VMEM) for x in state]
    result, _ = pl.pallas_call(
        finish,
        name="finish",
        out_shape=[jax.ShapeDtypeStruct(field.shape, f32), pltpu.VMEM(shared[1], f32)],
        in_specs=[vmem] * len(shared),
        out_specs=[hbm, vmem],
        input_output_aliases={1: 1},
        scratch_shapes=[pltpu.VMEM((2 * NQ, NY, NZ), f32), *inserts, dma((5,))],
        compiler_params=pltpu.CompilerParams(vmem_limit_bytes=VMEM_GRANT),
    )(*state)
    return result


def solution(mesh):
    spec = P("gx", "gy", "gz")
    return jax.shard_map(
        on_device, mesh=mesh, in_specs=(spec, spec), out_specs=spec, check_vma=False
    )
```

```python
import functools
import itertools
import types

import jax
import jax.numpy as jnp
from jax import lax
from jax.experimental import pallas as pl
from jax.experimental.pallas import tpu as pltpu
from jax.sharding import PartitionSpec as P

MESH = pl.DeviceIdType.MESH
SWEEPS = 3
NQ, NY, NZ = 8, 256, 128
TILES = NY // 8
ENDS = (0, TILES - 1)
TOP = 16
ROWS = NY + 2 * TOP
VECS = TILES // 8
COLS = 8 * VECS
SIXTH = 1.0 / 6.0
VMEM_GRANT = 24 << 20

EDGES = [d for d in itertools.product((-1, 0, 1), repeat=3) if sum(map(abs, d)) == 2]
FACES = [(0, 0, 1), (0, 0, -1), (0, 1, 0), (0, -1, 0), (1, 0, 0), (-1, 0, 0)]
MESSAGES = [d for d in EDGES if d[0] == 0] + [d for d in EDGES if d[0]] + FACES
X_FACES, Y_FACES, Z_FACES = FACES[4:], FACES[2:4], FACES[:2]
YZ_EDGES, XY_EDGES, XZ_EDGES = ([d for d in EDGES if d[a] == 0] for a in (0, 2, 1))


def when(cond, f):
    if cond is None:
        f()
    else:
        pl.when(cond)(f)


def cells(blk, red, sred, sblk, ql, qr, xq, qlo, qhi, sql, sqr, sx, merged, ins, xins, rins):
    gx = lax.axis_index("gx")
    low_wall, high_wall = gx == 0, gx == lax.axis_size("gx") - 1
    lane = lax.broadcasted_iota(jnp.int32, (8, NZ), 1)
    sub = lax.broadcasted_iota(jnp.int32, (8, NZ), 0)
    odd = jnp.bitwise_and(lane + sub, 1) == 1
    even_lane = jnp.bitwise_and(lane, 1) == 0
    first, last = lane == 0, lane == NZ - 1
    outer = jnp.logical_or(first, last)
    group = jnp.bitwise_and(lane, 15)
    half = jnp.right_shift(lane, 1)
    half_after = jnp.bitwise_and(half - 1, NZ // 2 - 1)

    def roll(x, shift):
        return pltpu.roll(x, shift, 1)

    def slot(t, q):
        return 8 * (t % 8) + q

    inside = jnp.where(odd, jnp.where(low_wall, 0.0, SIXTH), jnp.where(high_wall, 0.0, SIXTH))

    def swap(x):
        return jnp.where(jnp.bitwise_and(sub, 1) == 0, pltpu.roll(x, 7, 0), pltpu.roll(x, 1, 0))

    def columns(r, edges):
        for v in range(-1, VECS + 1) if edges else range(VECS):
            rows = pl.ds(8 * v + 8, 8)
            ins[rows] = jnp.where(even_lane, qr[r, rows], ql[r, rows])
        for v in range(VECS):
            here, rows = pl.ds(8 * v + 8, 8), pl.ds(8 * v, 8)
            c = ins[here]
            before = ins[rows] if edges or v > 0 else c
            after = ins[pl.ds(8 * v + 16, 8)] if edges or v < VECS - 1 else c
            back = roll(jnp.where(lane >= NZ - 16, before, c), 16)
            ahead = roll(jnp.where(lane < 16, after, c), NZ - 16)
            total = c + jnp.where(sub == 0, pltpu.roll(back, 1, 0), pltpu.roll(c, 1, 0))
            total = total + jnp.where(sub == 7, pltpu.roll(ahead, 7, 0), pltpu.roll(c, 7, 0))
            up, down = roll(c, NZ - 2), roll(c, 2)
            if edges:
                above = jnp.where(even_lane, xq[r, 1, 1], xq[r, 1, 0])
                below = jnp.where(even_lane, xq[r, 0, 1], xq[r, 0, 0])
                back = (NZ - 2 * v) % NZ
                below = roll(below, back)
                up = jnp.where(group >= 14, roll(above, 14 - 2 * v), up)
                down = jnp.where(group < 2, below, down)
                xins[rows] = jnp.where(odd, roll(above, back), below)
            total = total + jnp.where(odd, up, down)
            left, right = ql[r, here] + qlo[r, rows], qr[r, here] + qhi[r, rows]
            total = total + jnp.where(even_lane, roll(right, NZ - 1), roll(left, 1))
            total = total + jnp.where(even_lane, sqr[rows], sql[rows])
            rins[rows] = total * SIXTH

    def beside(c, edge, m):
        edge = roll(edge, NZ - 1 - 2 * m)
        return jnp.where(first, edge, roll(c, 1)) + jnp.where(last, edge, roll(c, NZ - 1))

    def around(ref, lead, row, edge, m):
        c = ref[(*lead, pl.ds(row, 8))]
        total = c + ref[(*lead, pl.ds(row - 1, 8))] + ref[(*lead, pl.ds(row + 1, 8))]
        return total + beside(c, edge, m)

    def red_tile(r, q, t):
        row = TOP + 8 * t
        rows = pl.ds(row, 8)
        c = blk[r, q + 1, rows]
        total = c + jnp.where(first, 0.0, roll(c, 1)) + jnp.where(last, 0.0, roll(c, NZ - 1))
        up = jnp.where(sub == 0, 0.0, pltpu.roll(c, 1, 0)) if t == 0 else blk[r, q + 1, pl.ds(row - 1, 8)]
        down = jnp.where(sub == 7, 0.0, pltpu.roll(c, 7, 0)) if t == TILES - 1 else blk[r, q + 1, pl.ds(row + 1, 8)]
        above = blk[r, q + 2, rows] if q < NQ - 1 else 0.0
        below = blk[r, q, rows] if q > 0 else 0.0
        total = total + up + down + jnp.where(odd, above, below)
        red[q + 1, rows] = (total + sred[q + 1, rows]) * SIXTH

    def complete_z(q, t):
        rows = pl.ds(TOP + 8 * t, 8)
        edge = roll(ins[pl.ds(8 * (t // 8) + 8, 8)], NZ - 1 - 2 * slot(t, q))
        red[q + 1, rows] = red[q + 1, rows] + jnp.where(outer, edge, 0.0) * SIXTH

    def red_beyond(r, q, t):
        rows = pl.ds(TOP + 8 * t, 8)
        total = around(blk, (r, q + 1), TOP + 8 * t, ins[pl.ds(8 * (t // 8) + 8, 8)], slot(t, q))
        total = total + jnp.where(odd, blk[r, q + 2, rows], blk[r, q, rows])
        red[q + 1, rows] = (total + sred[q + 1, rows]) * SIXTH

    def complete(r, q, t):
        row = TOP + 8 * t
        rows = pl.ds(row, 8)
        more = None
        if t == 0:
            more = jnp.where(sub == 0, blk[r, q + 1, pl.ds(row - 1, 8)], 0.0)
        if t == TILES - 1:
            more = jnp.where(sub == 7, blk[r, q + 1, pl.ds(row + 1, 8)], 0.0)
        side = None
        if q == 0:
            side = jnp.where(odd, 0.0, blk[r, 0, rows])
        if q == NQ - 1:
            side = jnp.where(odd, blk[r, 9, rows], 0.0)
        if side is not None:
            more = side if more is None else more + side
        if more is not None:
            red[q + 1, rows] = red[q + 1, rows] + more * SIXTH

    def halo_tiles(r, tiles):
        for t in tiles:
            row = TOP + 8 * t
            rows = pl.ds(row, 8)
            low, high = blk[r, 0, rows], blk[r, 9, rows]
            c, far = jnp.where(odd, high, low), jnp.where(odd, low, high)
            total = jnp.where(odd, blk[r, 0, pl.ds(row - 1, 8)], blk[r, 9, pl.ds(row - 1, 8)])
            total = total + jnp.where(odd, blk[r, 0, pl.ds(row + 1, 8)], blk[r, 9, pl.ds(row + 1, 8)])
            total = total + beside(c, xins[pl.ds(8 * (t // 8), 8)], slot(t, 0))
            total = total + far + jnp.where(odd, blk[r, 1, rows], blk[r, 8, rows])
            red[0, rows] = (total + sx[pl.ds(8 * t, 8)]) * inside

    def black_tile(r, q, t, final):
        rows = pl.ds(TOP + 8 * t, 8)
        total = around(red, (q + 1,), TOP + 8 * t, rins[pl.ds(8 * (t // 8), 8)], slot(t, q))
        above = (0 if q == NQ - 1 else q + 2) if isinstance(q, int) else q + 2
        total = total + jnp.where(odd, red[q, rows], red[above, rows])
        mine = pl.ds(8 * t, 8)
        value = (total + sblk[q, mine]) * SIXTH
        if final:
            other = red[q + 1, rows]
            merged[2 * q, mine] = jnp.where(odd, value, other)
            merged[2 * q + 1, mine] = jnp.where(odd, other, value)
        else:
            blk[r + 1, q + 1, rows] = value

    def finish_ends(r, final):
        for q in range(NQ):
            for t in (-1, TILES):
                red_beyond(r, q, t)
            for t in (0, 1, TILES - 2, TILES - 1):
                complete(r, q, t)
        halo_tiles(r, (0, 1, TILES - 2, TILES - 1))
        for q in range(NQ):
            for t in ENDS:
                black_tile(r, q, t, final)

    def finish_sides(r, final, ready=None):
        for q in (0, NQ - 1):
            for t in range(2, TILES - 2):
                complete(r, q, t)
        halo_tiles(r, range(2, TILES - 2))
        for n, q in enumerate((0, NQ - 1)):
            for t in range(1, TILES - 1):
                black_tile(r, q, t, final)
            if ready is not None:
                ready(n)

    return types.SimpleNamespace(**locals())


def kernel(
    field, source,
    blk, red, sred, sblk, ql, qr, xq, qlo, qhi, sql, sqr, sx, merged,
    fld, src, elo, ehi, xe, sqlo, sqhi, ins, xins, rins, sxs, sxd,
    load_sem, send_sem, recv_sem, ssend_sem, srecv_sem,
):
    def load(array, buffer, half, n):
        planes = pl.ds(4 * n, 4)
        return pltpu.make_async_copy(array.at[planes], buffer.at[planes], load_sem.at[half, n])

    for n in range(4):
        load(field, fld, 0, n).start()
    for n in range(4):
        load(source, src, 1, n).start()

    gx, gy, gz = (lax.axis_index(a) for a in ("gx", "gy", "gz"))
    nx, ny, nz = (lax.axis_size(a) for a in ("gx", "gy", "gz"))
    low_wall, high_wall = gx == 0, gx == nx - 1

    def device(d):
        return {
            "gx": gx + d[0],
            "gy": lax.rem(gy + d[1] + ny, ny),
            "gz": lax.rem(gz + d[2] + nz, nz),
        }

    def exists(d):
        if d[0] > 0:
            return gx < nx - 1
        if d[0] < 0:
            return gx > 0
        return None

    def opposite(d):
        return tuple(-v for v in d)

    def block_slices(d):
        dx, dy, _ = d
        sp, dp = ((8, 0) if dx > 0 else (1, 9)) if dx else (pl.ds(1, NQ), pl.ds(1, NQ))
        sr, dr = ((TOP + NY - 8, TOP - 8) if dy > 0 else (TOP, TOP + NY)) if dy else (TOP, TOP)
        n = 8 if dy else NY
        return (sp, pl.ds(sr, n)), (dp, pl.ds(dr, n))

    def refs(r, d):
        dx, dy, dz = d
        if dz == 0:
            s, t = block_slices(d)
            return blk.at[(r, *s)], blk.at[(r, *t)]
        col, dst = (qhi, ql) if dz > 0 else (qlo, qr)
        own = pl.ds(8, COLS)
        if dx:
            place = (r, 0 if dx > 0 else 1, 0 if dz > 0 else 1)
            return xe.at[place], xq.at[place]
        if dy:
            end, dr = (1, 0) if dy > 0 else (0, COLS + 8)
            return (ehi if dz > 0 else elo).at[r, end], dst.at[r, pl.ds(dr, 8)]
        return col.at[r], dst.at[r, own]

    def side(d):
        return 1 if d[0] > 0 else 2 if d[0] < 0 else 0

    def message(r, m):
        d = MESSAGES[m]
        s, t = refs(r, d)
        group = 3 if d in Z_FACES else side(d)
        return pltpu.make_async_remote_copy(
            src_ref=s, dst_ref=t, send_sem=send_sem.at[side(d)], recv_sem=recv_sem.at[r % 2, group],
            device_id=device(d), device_id_type=MESH,
        )

    def smessage(m):
        d = FACES[m]
        if d[2]:
            s, t = (sqhi, sql) if d[2] > 0 else (sqlo, sqr)
        elif d[0]:
            n = side(d) - 1
            s, t = sxs.at[n], sxd.at[n]
        else:
            s, t = block_slices(d)
            s, t = sred.at[s], sred.at[t]
        group = 3 if d in Z_FACES else side(d)
        return pltpu.make_async_remote_copy(
            src_ref=s, dst_ref=t, send_sem=ssend_sem.at[side(d)], recv_sem=srecv_sem.at[group],
            device_id=device(d), device_id_type=MESH,
        )

    def start(make, dirs, select):
        for m, d in enumerate(dirs):
            if d in select:
                when(exists(d), lambda m=m: make(m).start())

    def wait(sem, kib):
        some = fld.at[pl.ds(0, 2), pl.ds(0, kib)]
        pltpu.make_async_copy(some, some, sem).wait()

    SIDE_KIB = 128 + 4 * 4

    def wait_sides(sems, kib, sent):
        when(exists((1 if sent else -1, 0, 0)), lambda: wait(sems(1), kib))
        when(exists((-1 if sent else 1, 0, 0)), lambda: wait(sems(2), kib))

    def arrived_z(r):
        wait(recv_sem.at[r % 2, 3], 2 * 16)

    def arrived_rest(r):
        wait(recv_sem.at[r % 2, 0], 4 * 4 + 2 * 32)
        wait_sides(lambda g: recv_sem.at[r % 2, g], SIDE_KIB, False)

    def sent():
        wait(send_sem.at[0], 4 * 4 + 2 * 16 + 2 * 32)
        wait_sides(lambda g: send_sem.at[g], SIDE_KIB, True)

    def ssent():
        wait(ssend_sem.at[0], 2 * 16 + 2 * 32)
        wait_sides(lambda g: ssend_sem.at[g], 64, True)

    barrier = pltpu.get_barrier_semaphore()
    for d in MESSAGES:
        when(exists(d), lambda d=d: pl.semaphore_signal(barrier, inc=1, device_id=device(d), device_id_type=MESH))

    w = cells(blk, red, sred, sblk, ql, qr, xq, qlo, qhi, sql, sqr, sx, merged, ins, xins, rins)
    sub, odd, half, half_after = w.sub, w.odd, w.half, w.half_after
    roll, slot, swap = w.roll, w.slot, w.swap

    def collect(lo, hi, lead, t, q, value, rows=None):
        m = slot(t, q)
        turned = roll(value, jnp.bitwise_and(2 * m + 2, NZ - 1))
        rows = pl.ds(8 * (t // 8), 8) if rows is None else rows
        hi[(*lead, rows)] = jnp.where(half == m, turned, hi[(*lead, rows)])
        lo[(*lead, rows)] = jnp.where(half_after == m, turned, lo[(*lead, rows)])

    def collect_edges(r):
        for end, t in enumerate(ENDS):
            for q in range(NQ):
                collect(elo, ehi, (r, end), t, q, blk[r, q + 1, pl.ds(TOP + 8 * t, 8)], pl.ds(0, 8))
            elo[r, end] = roll(elo[r, end], NZ - 2)

    def settle(lo, lead):
        for v in range(VECS):
            rows = pl.ds(8 * v, 8)
            lo[(*lead, rows)] = roll(lo[(*lead, rows)], NZ - 2)

    def collect_xz(r):
        for place, pair in enumerate((NQ - 1, 0)):
            for z, col in enumerate((qhi, qlo)):
                piece = roll(col[r, pl.ds(0, 8)], (NZ - 2 * pair) % NZ)
                for v in range(1, VECS):
                    more = roll(col[r, pl.ds(8 * v, 8)], (2 * v - 2 * pair) % NZ)
                    piece = jnp.where(jnp.right_shift(w.group, 1) == v, more, piece)
                xe[r, place, z] = piece

    zero = jnp.zeros((ROWS, NZ), jnp.float32)

    def wall(pair, plane):
        for r in range(SWEEPS):
            blk[r, pair] = zero
            for z in range(2):
                xq[r, plane, z] = jnp.zeros((8, NZ), jnp.float32)
        sxd[0 if pair == 0 else 1] = jnp.zeros((NY // 2, NZ), jnp.float32)

    pl.when(low_wall)(lambda: wall(0, 0))
    pl.when(high_wall)(lambda: wall(9, 1))
    def pack_field(q, c):
        for t in range(TILES):
            rows = pl.ds(8 * t, 8)
            value = jnp.where(odd, fld[2 * q, rows], fld[2 * q + 1, rows])
            blk[0, q + 1, pl.ds(TOP + 8 * t, 8)] = value
            collect(qlo, qhi, (0,), t, q, value)
        return c

    def packed_field(n, c):
        load(field, fld, 0, n).wait()
        return pack_field(2 * n + 1, pack_field(2 * n, c))

    for n in range(4):
        packed_field(n, 0)
    collect_edges(0)
    settle(qlo, (0,))
    collect_xz(0)

    walls = jnp.where(jnp.logical_or(low_wall, high_wall), 1, 0)
    pl.semaphore_wait(barrier, len(MESSAGES) - 5 * walls)
    start(functools.partial(message, 0), MESSAGES, EDGES + Z_FACES + Y_FACES)

    def pack_source(q, c):
        for t in range(TILES):
            rows = pl.ds(8 * t, 8)
            even_plane, odd_plane = src[2 * q, rows], src[2 * q + 1, rows]
            value = jnp.where(odd, odd_plane, even_plane)
            sred[q + 1, pl.ds(TOP + 8 * t, 8)] = value
            sblk[q, rows] = jnp.where(odd, even_plane, odd_plane)
            collect(sqlo, sqhi, (), t, q, value)
        return c

    def packed_source(n, c):
        load(source, src, 1, n).wait()
        return pack_source(2 * n + 1, pack_source(2 * n, c))

    for n in range(4):
        packed_source(n, 0)
    settle(sqlo, ())
    start(smessage, FACES, Z_FACES + Y_FACES)
    start(functools.partial(message, 0), MESSAGES, X_FACES)
    for t in range(TILES // 2):
        near, away = pl.ds(TOP + 8 * t, 8), pl.ds(TOP + 8 * t + NY // 2, 8)
        sxs[0, pl.ds(8 * t, 8)] = jnp.where(odd, sred[NQ, near], swap(sred[NQ, away]))
        sxs[1, pl.ds(8 * t, 8)] = jnp.where(odd, swap(sred[1, away]), sred[1, near])
    start(smessage, FACES, X_FACES)

    def sweep(r, final):
        for q in range(NQ):
            for t in range(TILES):
                w.red_tile(r, q, t)
        arrived_z(r)
        pl.when(r == 0)(lambda: wait(srecv_sem.at[3], 2 * 16))

        w.columns(r, False)

        for q in range(NQ):
            for t in range(TILES):
                w.complete_z(q, t)

        def black_inner(n, c):
            for q in (3 * n + 1, 3 * n + 2, 3 * n + 3):
                for t in range(1, TILES - 1):
                    w.black_tile(r, q, t, final)
            return c

        black_inner(0, 0)
        black_inner(1, 0)
        if not final:
            for t in range(1, TILES - 1):
                for q in range(1, NQ - 1):
                    collect(qlo, qhi, (r + 1,), t, q, blk[r + 1, q + 1, pl.ds(TOP + 8 * t, 8)])

        arrived_rest(r)

        @pl.when(r == 0)
        def _():
            wait(srecv_sem.at[0], 2 * 32)
            wait_sides(lambda g: srecv_sem.at[g], 64, False)
            for t in range(TILES // 2):
                low, high = sxd[0, pl.ds(8 * t, 8)], sxd[1, pl.ds(8 * t, 8)]
                sx[pl.ds(8 * t, 8)] = jnp.where(odd, low, high)
                sx[pl.ds(8 * t + NY // 2, 8)] = swap(jnp.where(odd, high, low))

        sent()
        if final:
            return
        w.columns(r, True)
        w.finish_ends(r, False)
        after = functools.partial(message, r + 1)
        collect_edges(r + 1)
        start(after, MESSAGES, YZ_EDGES + XY_EDGES + Y_FACES)
        w.finish_sides(r, False)
        for t in range(TILES):
            for q in range(NQ) if t in ENDS else (0, NQ - 1):
                collect(qlo, qhi, (r + 1,), t, q, blk[r + 1, q + 1, pl.ds(TOP + 8 * t, 8)])
        settle(qlo, (r + 1,))
        start(after, MESSAGES, Z_FACES)
        collect_xz(r + 1)
        start(after, MESSAGES, XZ_EDGES + X_FACES)

    def sweeps(r, c):
        sweep(r, False)
        return c

    lax.fori_loop(0, SWEEPS - 1, sweeps, 0)
    sweep(SWEEPS - 1, True)
    ssent()


def finish(
    blk, red_in, sred, sblk, ql, qr, xq, qlo, qhi, sql, sqr, sx, merged, out, red,
    late, ins, xins, rins, sem,
):
    del red_in
    w = cells(blk, red, sred, sblk, ql, qr, xq, qlo, qhi, sql, sqr, sx, late, ins, xins, rins)

    def store(n):
        planes, rows = [
            (pl.ds(2, 2 * NQ - 4), pl.ds(8, NY - 16)),
            (pl.ds(2, 2 * NQ - 4), pl.ds(0, 8)),
            (pl.ds(2, 2 * NQ - 4), pl.ds(NY - 8, 8)),
            (pl.ds(0, 2), pl.ds(0, NY)),
            (pl.ds(2 * NQ - 2, 2), pl.ds(0, NY)),
        ][n]
        origin = merged if n == 0 else late
        return pltpu.make_async_copy(origin.at[planes, rows], out.at[planes, rows], sem.at[n])

    store(0).start()
    r = SWEEPS - 1
    w.columns(r, True)
    w.finish_ends(r, True)
    store(1).start()
    store(2).start()
    w.finish_sides(r, True, lambda n: store(3 + n).start())
    for n in range(5):
        store(n).wait()


def on_device(field, source):
    f32 = jnp.float32
    dma = pltpu.SemaphoreType.DMA
    columns = (COLS, NZ)
    shared = [
        (SWEEPS, NQ + 2, ROWS, NZ),
        (NQ + 1, ROWS, NZ),
        (NQ + 2, ROWS, NZ),
        (NQ, NY, NZ),
        (SWEEPS, COLS + 16, NZ),
        (SWEEPS, COLS + 16, NZ),
        (SWEEPS, 2, 2, 8, NZ),
        (SWEEPS, *columns),
        (SWEEPS, *columns),
        columns,
        columns,
        (NY, NZ),
        (2 * NQ, NY, NZ),
    ]
    vmem, hbm = (pl.BlockSpec(memory_space=m) for m in (pltpu.VMEM, pltpu.HBM))
    inserts = [pltpu.VMEM(shape, f32) for shape in ((COLS + 16, NZ), columns, columns)]
    field, source = (pltpu.with_memory_space_constraint(x, pltpu.HBM) for x in (field, source))
    state = pl.pallas_call(
        kernel,
        name="smooth",
        out_shape=[pltpu.VMEM(shape, f32) for shape in shared],
        in_specs=[hbm] * 2,
        out_specs=[vmem] * len(shared),
        scratch_shapes=[
            pltpu.VMEM((2 * NQ, NY, NZ), f32),
            pltpu.VMEM((2 * NQ, NY, NZ), f32),
            pltpu.VMEM((SWEEPS, 2, 8, NZ), f32),
            pltpu.VMEM((SWEEPS, 2, 8, NZ), f32),
            pltpu.VMEM((SWEEPS, 2, 2, 8, NZ), f32),
            pltpu.VMEM(columns, f32),
            pltpu.VMEM(columns, f32),
            *inserts,
            pltpu.VMEM((2, NY // 2, NZ), f32),
            pltpu.VMEM((2, NY // 2, NZ), f32),
            dma((2, 4)),
            dma((3,)),
            dma((2, 4)),
            dma((3,)),
            dma((4,)),
        ],
        compiler_params=pltpu.CompilerParams(
            collective_id=0, has_side_effects=True, vmem_limit_bytes=VMEM_GRANT
        ),
    )(field, source)
    state = [pltpu.with_memory_space_constraint(x, pltpu.VMEM) for x in state]
    result, _ = pl.pallas_call(
        finish,
        name="finish",
        out_shape=[jax.ShapeDtypeStruct(field.shape, f32), pltpu.VMEM(shared[1], f32)],
        in_specs=[vmem] * len(shared),
        out_specs=[hbm, vmem],
        input_output_aliases={1: 1},
        scratch_shapes=[pltpu.VMEM((2 * NQ, NY, NZ), f32), *inserts, dma((5,))],
        compiler_params=pltpu.CompilerParams(vmem_limit_bytes=VMEM_GRANT),
    )(*state)
    return result


def solution(mesh):
    spec = P("gx", "gy", "gz")
    return jax.shard_map(
        on_device, mesh=mesh, in_specs=(spec, spec), out_specs=spec, check_vma=False
    )
```
